32 devices in a mesh: flow: 16 (over z, y, x), group: 2 (over core).
Axes of the slice: x: 2, y: 2, z: 4, core: 2. Of those that a mesh axis runs over, the one named last changes fastest.
Arguments:
- density: float32 [64, 32, 256], P('flow', 'group'), may hold values from 0.8 to 1.2
- velocity: float32 [3, 64, 32, 256], P(None, 'flow', 'group'), may hold values from -0.5 to 0.5
- pressure: float32 [64, 32, 256], P('flow', 'group'), may hold values from 0.7 to 1.3
- wave_state: float32 [4, 8, 8, 8, 4096], P(None, None, None, None, ('flow', 'group')), may hold values from -1.8 to 1.8
- tables: float32 [4, 512, 512], replicated, may hold values from -0.75 to 0.75
- margin_element: int32 [32, 64], P(('flow', 'group')), may hold values from 0 to 4095, as said below
- margin_block: int32 [32, 64], P(('flow', 'group')), may hold values from 0 to 31
- margin_table: int32 [32, 64], P(('flow', 'group')), may hold values from 0 to 3
Outputs:
- flow_state: float32 [5, 64, 32, 256], P(None, 'flow', 'group')
- wave_out: float32 [4, 8, 8, 8, 4096], P(None, None, None, None, ('flow', 'group'))
- forcing: float32 [3, 8, 8, 8, 4096], P(None, None, None, None, ('flow', 'group'))
The draws below stay inside these ranges and needn't reach their ends.
Inputs may be any that keep to these rules, and one draw needn't show every extreme that they name: `margin_element`: global element ids; element e belongs to the device at position e // 128 along flow then group. In every device's row at most 4 entries name elements of one owner, and some owner receives exactly 4 entries from it.
All inputs are finite; a program needn't handle non-finite values.
Results may differ from the reference program's by a relative error of at most 0.0003.
Values sent between devices are 32-bit elements; how exact they have to be, the bound alone decides.
A program may use at most 128 MiB of HBM per device.

```python
import jax
import jax.numpy as jnp
import numpy as np
from jax import lax

NP = 8
CX = 4
CY = 16
NZ = 256
EY = 8
EZ = 16
CAP = 4
NW = 4
STEPS = 2
OV_DEV = 64
NX = 64
NY = 32
NBLK = 32
ELEMENTS = 4096
N_FLOW = 16
N_GROUP = 2


def draw_margin_element(key, part):
    devices = N_FLOW * N_GROUP
    slot_total = devices * CAP
    center_key, choose_key = jax.random.split(jax.random.fold_in(key, 11))
    center = jax.random.randint(center_key, (), 0, devices)
    hot_width = max(devices // 16, 2)

    def one_sender(sender_key, sender):
        sub_keys = jax.random.split(sender_key, 3)
        owner_index = jnp.arange(slot_total, dtype=jnp.int32) // CAP
        offset = (owner_index - center) % devices
        priority = jax.random.randint(sub_keys[0], (slot_total,), 0, 2)
        priority = jnp.where(offset < hot_width, 2, priority)
        priority = jnp.where(owner_index == (center + 3 * sender + hot_width) % devices, 3, priority)
        tiebreak = jax.random.permutation(sub_keys[1], slot_total)
        scores = priority * (slot_total + 1) + tiebreak
        chosen = jnp.sort(jax.lax.top_k(scores, OV_DEV)[1])
        element = chosen // CAP * (EY * EZ) + jax.random.randint(sub_keys[2], (OV_DEV,), 0, EY * EZ)
        return element.astype(jnp.int32)
    sender_keys = jax.random.split(choose_key, devices)
    return jax.vmap(one_sender)(sender_keys, jnp.arange(devices, dtype=jnp.int32))


def plant(drawn, stream_key, low, top_value):
    spot = [jax.random.randint(jax.random.fold_in(stream_key, axis), (), 0, length) for axis, length in enumerate(drawn.shape)]
    longest = drawn.shape.index(max(drawn.shape))
    beside = spot[:longest] + [(spot[longest] + 1) % drawn.shape[longest]] + spot[longest + 1:]
    return drawn.at[tuple(spot)].set(low).at[tuple(beside)].set(top_value)


def levels(key, shape, cuts, low, high):
    def one(position, shards_of):
        steps = jax.random.uniform(jax.random.fold_in(jax.random.fold_in(key, 6), position), (shards_of,), jnp.float32, low / len(cuts), high / len(cuts))
        return jnp.repeat(jnp.exp(steps), shape[position] // shards_of).reshape((-1,) + (1,) * (len(shape) - position - 1))

    factor_of = one(*cuts[0])
    for cut in cuts[1:]:
        factor_of = factor_of * one(*cut)
    return factor_of


def centred(rng, shape, spread, reach, cuts=(), kind=jnp.bfloat16):
    values = jax.random.normal(rng, shape, jnp.float32) * spread
    if len(cuts) > 0:
        values = levels(rng, shape, cuts, -0.22, 0.18) * values
    return jnp.clip(values, min=-reach, max=reach).astype(kind)


def setup_inputs(seed: int = 0) -> dict:
    streams_of = jax.random.split(jax.random.key(seed), 9)
    density = jnp.clip(0.8 + 0.40000004 * jax.random.uniform(streams_of[0], (NX, NY, NZ), jnp.float32) ** levels(streams_of[0], (NX, NY, NZ), ((0, 16), (1, 2)), -0.2, 0.2), 0.8, 1.2)
    velocity = jnp.clip(jax.random.uniform(streams_of[1], (3, NX, NY, NZ), jnp.float32, -0.5, 0.5) * levels(streams_of[1], (3, NX, NY, NZ), ((1, 16), (2, 2)), -0.4, 0.0), -0.5, 0.5)
    pressure = jnp.clip(0.7 + 0.59999996 * jax.random.uniform(streams_of[2], (NX, NY, NZ), jnp.float32) ** levels(streams_of[2], (NX, NY, NZ), ((0, 16), (1, 2)), -0.2, 0.2), 0.7, 1.3)
    wave_state = centred(streams_of[3], (4, NP, NP, NP, ELEMENTS), 0.3, 1.8, ((4, 32),), jnp.float32)
    tables = centred(streams_of[4], (NW, NP**3, NP**3), 0.125, 0.75, (), jnp.float32)
    margin_element = draw_margin_element(jax.random.fold_in(streams_of[8], 71), 0)
    margin_block = plant(jax.random.randint(streams_of[6], (N_FLOW * N_GROUP, OV_DEV), 0, NBLK), jax.random.fold_in(streams_of[6], 1), 0, NBLK - 1).astype(jnp.int32)
    margin_table = plant(jax.random.randint(streams_of[7], (N_FLOW * N_GROUP, OV_DEV), 0, NW), jax.random.fold_in(streams_of[7], 1), 0, NW - 1).astype(jnp.int32)
    return {"density": density, "velocity": velocity, "pressure": pressure, "wave_state": wave_state, "tables": tables, "margin_element": margin_element, "margin_block": margin_block, "margin_table": margin_table}


GAMMA = 1.4
DT_FLOW = 0.08
ACOUSTIC_STEP = 0.01
MAXIMUM_DEGREE = lax.Precision.HIGHEST

def legendre_pair(quadrature_nodes, degree):
    previous = np.ones(quadrature_nodes.shape[0])
    current = quadrature_nodes * 1.0
    for order in range(2, degree + 1):
        previous, current = (current, ((2 * order - 1) * quadrature_nodes * current - (order - 1) * previous) / order)
    return (previous, current)

def lobatto(point_count):
    degree = point_count - 1
    quadrature_nodes = -np.cos(np.pi * np.arange(point_count) / degree)
    for sweep in range(60):
        previous, current = legendre_pair(quadrature_nodes, degree)
        quadrature_nodes = quadrature_nodes - (quadrature_nodes * current - previous) / (point_count * current)
    previous, values = legendre_pair(quadrature_nodes, degree)
    quadrature_weights = 2.0 / (degree * (degree + 1) * values ** 2)
    identity = np.eye(point_count)
    differ = quadrature_nodes[:, None] - quadrature_nodes[None, :] + identity
    matrix = values[:, None] / values[None, :] / differ * (1.0 - identity)
    matrix[0, 0] = -degree * (degree + 1) / 4.0
    matrix[-1, -1] = degree * (degree + 1) / 4.0
    return (matrix, float(quadrature_weights[0]))

def physical(fields):
    density = fields[0]
    velocity = fields[1:4] / density
    pressure = (GAMMA - 1.0) * (fields[4] - 0.5 * density * lax.optimization_barrier(jnp.sum(velocity * velocity, axis=0)))
    return (density, velocity, pressure)

def euler_flux(fields, velocity, pressure, direction):
    normal = velocity[direction]
    components = [fields[0] * normal]
    for column in range(3):
        product = fields[1 + column] * normal
        if column == direction:
            product = product + pressure
        components.append(product)
    components.append((fields[4] + pressure) * normal)
    return jnp.stack(components)

def rusanov(left_side, right_side, direction):
    left_rho, left_vel, left_pre = physical(left_side)
    right_rho, right_vel, right_pre = physical(right_side)
    wave_speed = jnp.maximum(jnp.abs(left_vel[direction]) + jnp.sqrt(GAMMA * left_pre / left_rho), jnp.abs(right_vel[direction]) + jnp.sqrt(GAMMA * right_pre / right_rho))
    return 0.5 * (euler_flux(left_side, left_vel, left_pre, direction) + euler_flux(right_side, right_vel, right_pre, direction)) - 0.5 * wave_speed * (right_side - left_side)

def flow_rate(fields):
    tendency = jnp.zeros_like(fields)
    for direction in range(3):
        axis_index = direction + 1
        face_flux = rusanov(fields, jnp.roll(fields, -1, axis_index), direction)
        tendency = tendency - (face_flux - jnp.roll(face_flux, 1, axis_index))
    return tendency

def lamb_vector(fields):
    velocity = fields[1:4] / fields[0]
    slope_x = 0.5 * (jnp.roll(velocity, -1, 1) - jnp.roll(velocity, 1, 1))
    slope_y = 0.5 * (jnp.roll(velocity, -1, 2) - jnp.roll(velocity, 1, 2))
    slope_z = 0.5 * (jnp.roll(velocity, -1, 3) - jnp.roll(velocity, 1, 3))
    curl_x = slope_y[2] - slope_z[1]
    curl_y = slope_z[0] - slope_x[2]
    curl_z = slope_x[1] - slope_y[0]
    return jnp.stack([curl_y * velocity[2] - curl_z * velocity[1], curl_z * velocity[0] - curl_x * velocity[2], curl_x * velocity[1] - curl_y * velocity[0]])

def derivative(values, derive, direction):
    forms = ('ai,ijke->ajke', 'aj,ijke->iake', 'ak,ijke->ijae')
    return jnp.einsum(forms[direction], derive, values, precision=MAXIMUM_DEGREE)

def place_lifts(lower_lift, upper_lift, direction, point_count):
    middle_shape = list(upper_lift.shape)
    middle_shape.insert(direction, point_count - 2)
    middle = jnp.zeros(middle_shape, upper_lift.dtype)
    return jnp.concatenate([jnp.expand_dims(lower_lift, direction), middle, jnp.expand_dims(upper_lift, direction)], axis=direction)

def wave_rate(wave_field, forcing, upper_of, lower_of):
    point_count = wave_field.shape[1]
    matrix, end_weight = lobatto(point_count)
    derive = jnp.asarray(matrix, jnp.float32)
    pressure = wave_field[0]
    pressure_rate = jnp.zeros_like(pressure)
    velocity_tendency = []
    last = point_count - 1
    for direction in range(3):
        normal = wave_field[1 + direction]
        lower_face = jnp.stack([jnp.take(pressure, 0, axis=direction), jnp.take(normal, 0, axis=direction)])
        upper_face = jnp.stack([jnp.take(pressure, last, axis=direction), jnp.take(normal, last, axis=direction)])
        above_face = upper_of(lower_face, direction)
        below_face = lower_of(upper_face, direction)
        upper_pressure_flux = 0.5 * (upper_face[1] + above_face[1]) - 0.5 * (above_face[0] - upper_face[0])
        upper_normal_flux = 0.5 * (upper_face[0] + above_face[0]) - 0.5 * (above_face[1] - upper_face[1])
        lower_pressure_flux = 0.5 * (below_face[1] + lower_face[1]) - 0.5 * (lower_face[0] - below_face[0])
        lower_normal_flux = 0.5 * (below_face[0] + lower_face[0]) - 0.5 * (lower_face[1] - below_face[1])
        pressure_lift = place_lifts((lower_pressure_flux - lower_face[1]) / end_weight, -(upper_pressure_flux - upper_face[1]) / end_weight, direction, point_count)
        normal_lift = place_lifts((lower_normal_flux - lower_face[0]) / end_weight, -(upper_normal_flux - upper_face[0]) / end_weight, direction, point_count)
        pressure_rate = pressure_rate - derivative(normal, derive, direction) + pressure_lift
        velocity_tendency.append(-derivative(pressure, derive, direction) + normal_lift + forcing[direction])
    return jnp.stack([pressure_rate] + velocity_tendency)

def runge_kutta(start, rate, step_size):
    first_section = start + step_size * rate(start)
    second_section = 0.75 * start + 0.25 * (first_section + step_size * rate(first_section))
    return start / 3.0 + 2.0 / 3.0 * (second_section + step_size * rate(second_section))

def project(source, tables, margin_element, margin_block, margin_table):
    devices = N_FLOW * N_GROUP
    node_count = NP ** 3
    sorted_entries = source.reshape(3, N_FLOW, CX, N_GROUP, CY, NZ).transpose(0, 1, 3, 2, 4, 5)
    sorted_entries = sorted_entries.reshape(3, devices, NBLK, node_count)
    mapped_values = jnp.einsum('cdbn,tnm->tcdbm', sorted_entries, tables, precision=MAXIMUM_DEGREE)
    owners = jnp.broadcast_to(jnp.arange(devices, dtype=jnp.int32)[:, None], margin_block.shape)
    pieces = mapped_values[margin_table, :, owners, margin_block, :]
    summed = jax.ops.segment_sum(pieces.reshape(devices * OV_DEV, 3 * node_count), margin_element.reshape(-1), num_segments=ELEMENTS)
    return summed.reshape(ELEMENTS, 3, NP, NP, NP).transpose(1, 2, 3, 4, 0)

def shifted(faces, direction, offset):
    grid_view = faces.reshape(faces.shape[:3] + (N_FLOW * N_GROUP, EY, EZ))
    return jnp.roll(grid_view, offset, 3 + direction).reshape(faces.shape)

def reference(density, velocity, pressure, wave_state, tables, margin_element, margin_block, margin_table):
    momentum = density[None] * velocity
    energy = pressure / (GAMMA - 1.0) + 0.5 * density * lax.optimization_barrier(jnp.sum(velocity * velocity, axis=0))
    fields = jnp.concatenate([density[None], momentum, energy[None]], axis=0)
    wave_field = wave_state
    forcing = jnp.zeros((3, NP, NP, NP, ELEMENTS), jnp.float32)
    for step_index in range(STEPS):
        forcing = project(lamb_vector(fields), tables, margin_element, margin_block, margin_table)
        fields = runge_kutta(fields, flow_rate, DT_FLOW)
        wave_field = runge_kutta(wave_field, lambda current: wave_rate(current, forcing, lambda faces, direction: shifted(faces, direction, -1), lambda faces, direction: shifted(faces, direction, 1)), ACOUSTIC_STEP)
    return (fields, wave_field, forcing)
```

```python
import jax
import jax.numpy as jnp
import numpy as np
from jax import lax
from jax.experimental import pallas as pl
from jax.experimental.pallas import tpu as pltpu
from jax.sharding import PartitionSpec as P

EZ = 16
CAP = 4
STEPS = 2

GAMMA = 1.4
DT_FLOW = 0.08
ACOUSTIC_STEP = 0.01
F32, BF16 = jnp.float32, jnp.bfloat16
KEEP = (0.0, 0.75, 1.0 / 3.0)
GAIN = (1.0, 0.25, 2.0 / 3.0)


def legendre_pair(quadrature_nodes, degree):
    previous = np.ones(quadrature_nodes.shape[0])
    current = quadrature_nodes * 1.0
    for order in range(2, degree + 1):
        previous, current = (
            current,
            ((2 * order - 1) * quadrature_nodes * current - (order - 1) * previous) / order,
        )
    return (previous, current)


def lobatto(point_count):
    degree = point_count - 1
    quadrature_nodes = -np.cos(np.pi * np.arange(point_count) / degree)
    for sweep in range(60):
        previous, current = legendre_pair(quadrature_nodes, degree)
        quadrature_nodes = quadrature_nodes - (quadrature_nodes * current - previous) / (
            point_count * current
        )
    previous, values = legendre_pair(quadrature_nodes, degree)
    quadrature_weights = 2.0 / (degree * (degree + 1) * values**2)
    identity = np.eye(point_count)
    differ = quadrature_nodes[:, None] - quadrature_nodes[None, :] + identity
    matrix = values[:, None] / values[None, :] / differ * (1.0 - identity)
    matrix[0, 0] = -degree * (degree + 1) / 4.0
    matrix[-1, -1] = degree * (degree + 1) / 4.0
    return (matrix, float(quadrature_weights[0]))


def iota(shape, axis):
    return lax.broadcasted_iota(jnp.int32, shape, axis)


def split(value):
    high = value.astype(BF16)
    return high, (value - high.astype(F32)).astype(BF16)


def dot(a, b):
    return jnp.dot(a, b, preferred_element_type=F32)


def primitive(state):
    inverse = 1.0 / state[0]
    vel = [state[1 + d] * inverse for d in range(3)]
    square = vel[0] * vel[0] + vel[1] * vel[1] + vel[2] * vel[2]
    pressure = (GAMMA - 1.0) * (state[4] - 0.5 * state[0] * square)
    return vel, pressure, jnp.sqrt(GAMMA * pressure * inverse)


def flux_of(state, prim, d):
    vel, pressure, sound = prim
    normal = vel[d]
    parts = [state[0] * normal]
    for c in range(3):
        product = state[1 + c] * normal
        parts.append(product + pressure if c == d else product)
    parts.append((state[4] + pressure) * normal)
    return parts, jnp.abs(normal) + sound


def face(left, right, left_flux, right_flux, left_speed, right_speed):
    speed = jnp.maximum(left_speed, right_speed)
    return [
        0.5 * (left_flux[c] + right_flux[c]) - 0.5 * speed * (right[c] - left[c])
        for c in range(5)
    ]


def along(cell, prim, d, axis):
    size = cell[0].shape[axis]
    flux, speed = flux_of(cell, prim, d)
    back = lambda v: pltpu.roll(v, size - 1, axis)
    upper = face(
        cell, [back(v) for v in cell], flux, [back(v) for v in flux], speed, back(speed)
    )
    return [upper[c] - pltpu.roll(upper[c], 1, axis) for c in range(5)]


def tall_of(own, above, below):
    row = iota(above.shape, 0)
    return jnp.concatenate([own, jnp.where(row < above.shape[0] // 2, above, below)], axis=0)


def flow_stage(src, above, below, finish):
    planes, rows = src.shape[1] - 2, src.shape[2]

    def load(p):
        return [src[c, p] for c in range(5)]

    def x_side(p):
        cell = load(p)
        flux, speed = flux_of(cell, primitive(cell), 0)
        return cell, flux, speed

    def x_face(p):
        left, right = x_side(p), x_side(p + 1)
        return face(left[0], right[0], left[1], right[1], left[2], right[2])

    def body(p, lower):
        upper = x_face(p + 1)
        tall = [tall_of(src[c, p + 1], above[c, p], below[c, p]) for c in range(5)]
        prim = primitive(tall)
        dy = along(tall, prim, 1, 0)
        cell = [v[:rows] for v in tall]
        prim = ([v[:rows] for v in prim[0]], prim[1][:rows], prim[2][:rows])
        dz = along(cell, prim, 2, 1)
        for c in range(5):
            rate = -(upper[c] - lower[c]) - dy[c][:rows] - dz[c]
            finish(p, c, cell[c] + DT_FLOW * rate)
        return tuple(upper)

    lax.fori_loop(0, planes, body, tuple(x_face(0)))


def lamb(src, above, below, out):
    planes, rows, columns = src.shape[1] - 2, src.shape[2], src.shape[3]

    def body(p, _):
        density = tall_of(src[0, p + 1], above[0, p], below[0, p])
        inverse = 1.0 / density
        tall = [
            tall_of(src[1 + d, p + 1], above[1 + d, p], below[1 + d, p]) * inverse
            for d in range(3)
        ]
        size = tall[0].shape[0]
        slope_y = [
            0.5 * (pltpu.roll(v, size - 1, 0) - pltpu.roll(v, 1, 0))[:rows] for v in tall
        ]
        vel = [v[:rows] for v in tall]
        slope_z = [0.5 * (pltpu.roll(v, columns - 1, 1) - pltpu.roll(v, 1, 1)) for v in vel]
        after, before = 1.0 / src[0, p + 2], 1.0 / src[0, p]
        slope_x = [
            0.5 * (src[1 + d, p + 2] * after - src[1 + d, p] * before) for d in range(3)
        ]
        curl_x = slope_y[2] - slope_z[1]
        curl_y = slope_z[0] - slope_x[2]
        curl_z = slope_x[1] - slope_y[0]
        result = [
            curl_y * vel[2] - curl_z * vel[1],
            curl_z * vel[0] - curl_x * vel[2],
            curl_x * vel[1] - curl_y * vel[0],
        ]
        for d in range(3):
            for q in range(out.shape[2]):
                out[d, p, q] = result[d][:, q * 128 : (q + 1) * 128]
        return 0

    lax.fori_loop(0, planes, body, 0)


def split_tables(tables, high, low):
    count, depth, _ = tables.shape
    step = 64

    def body(i, _):
        t = i // (depth // step)
        at = pl.ds(pl.multiple_of((i % (depth // step)) * step, step), step)
        h, l = split(tables[t, at, :])
        high[t, at, :] = h
        low[t, at, :] = l
        return 0

    lax.fori_loop(0, count * (depth // step), body, 0)


def rows_of_slots(source, high, low, pick, mapped_high, mapped_low, send):
    _, planes, chunks, rows, width = source.shape
    columns = chunks * width
    table_count, depth, nodes = high.shape
    per = depth // columns
    strip = rows // per
    blocks = planes * strip
    half = 3 * nodes // 2
    pieces = []
    for y in range(3):
        for p in range(planes):
            pieces.append(
                jnp.concatenate(
                    [
                        source[y, p, q, pl.ds(r, strip, stride=per), :]
                        for r in range(per)
                        for q in range(chunks)
                    ],
                    axis=1,
                )
            )
    left_high, left_low = split(jnp.concatenate(pieces, axis=0))
    both = jnp.concatenate([left_high, left_low], axis=0)
    count = 3 * blocks

    def body(t, _):
        wide = dot(both, high[t])
        out = wide[:count] + wide[count:] + dot(left_high, low[t])
        for side in range(2):
            at = pl.ds(pl.multiple_of(side * table_count * blocks + t * blocks, blocks), blocks)
            for y in range(3):
                begin, end = max(y * nodes, side * half), min((y + 1) * nodes, (side + 1) * half)
                if begin < end:
                    value = out[y * blocks : (y + 1) * blocks, begin - y * nodes : end - y * nodes]
                    h, l = split(value)
                    mapped_high[at, begin - side * half : end - side * half] = h
                    mapped_low[at, begin - side * half : end - side * half] = l
        return 0

    lax.fori_loop(0, table_count, body, 0)
    send[...] = dot(pick[...], mapped_high[...]) + dot(pick[...], mapped_low[...])


def routes(element, block, table, blocks, table_count, local_count, devices, pick, label):
    entries = element.shape[1]
    shift = local_count.bit_length() - 1
    assert 1 << shift == local_count
    owner = lax.shift_right_logical(element, shift)
    local_index = element - lax.shift_left(owner, shift)
    column = table * blocks + block
    square = (entries, entries)
    row = jnp.broadcast_to(owner, square)
    turned = jnp.sum(jnp.where(iota(square, 0) == iota(square, 1), row, 0), axis=1, keepdims=True)
    earlier = (turned == row) & (iota(square, 0) < iota(square, 1))
    rank = jnp.sum(jnp.where(earlier, 1, 0), axis=0, keepdims=True)
    slot = owner * CAP + rank
    high = 2 * CAP
    lines = devices * high
    line = iota((lines, entries), 0)
    named = (line // high) * CAP + line % CAP
    hit = named == slot
    labels = jnp.sum(jnp.where(hit, local_index + 1, 0), axis=1, keepdims=True) - 1
    picked = jnp.sum(jnp.where(hit, column + 1, 0), axis=1, keepdims=True) - 1
    label[...] = jnp.broadcast_to(labels, label.shape)
    shape = pick.shape
    side = (iota(shape, 0) // CAP) % 2
    chosen = picked + side * (table_count * blocks)
    on = (iota(shape, 1) == chosen) & (picked >= 0)
    pick[...] = jnp.where(on, 1.0, 0.0).astype(BF16)


def place_of(label, place):
    shape = label.shape
    lines, lanes = shape
    side = (iota(shape, 0) // CAP) % 2
    hit = label[...] == iota(shape, 1)
    for s in range(2):
        place[:, s * lanes : (s + 1) * lanes] = jnp.where(hit & (side == s), 1.0, 0.0).astype(BF16)


def add_up(received, place, forcing):
    parts, lanes = forcing.shape[0] // 2, forcing.shape[-1]
    high, low = split(received[...].T)
    total = dot(high, place[...]) + dot(low, place[...])
    for s in range(2):
        forcing[s * parts : (s + 1) * parts] = total[:, s * lanes : (s + 1) * lanes].reshape(
            (parts,) + forcing.shape[1:]
        )


def halves(matrix):
    n = matrix.shape[0]
    turned = matrix[: n // 2, ::-1][:, : n // 2]
    own = matrix[: n // 2, : n // 2]
    return 0.5 * (own + turned), 0.5 * (own - turned)


def derive(values, even, odd):
    n = len(values)
    h = n // 2
    sums = [values[m] + values[n - 1 - m] for m in range(h)]
    gaps = [values[m] - values[n - 1 - m] for m in range(h)]
    out = [None] * n
    for a in range(h):
        alpha = sum(float(even[a, m]) * sums[m] for m in range(h))
        beta = sum(float(odd[a, m]) * gaps[m] for m in range(h))
        out[a] = beta + alpha
        out[n - 1 - a] = beta - alpha
    return out


def wave_main(start, cur, forcing, out, partial, edge, dcol, matrix, lift, stage, forced):
    keep, gain = KEEP[stage], GAIN[stage]
    n, lanes = cur.shape[1], cur.shape[-1]
    last = n - 1
    even, odd = halves(matrix)
    node = iota((n, lanes), 0)
    z = iota((n, lanes), 1) % EZ
    turn = lambda v, by: pltpu.roll(v, by % lanes, v.ndim - 1)

    def store(f, i, j, rate):
        value = gain * cur[f, i, j] + (gain * ACOUSTIC_STEP) * rate
        if keep:
            value = keep * start[f, i, j] + value
        out[f, i, j] = value

    def push(d, i, j):
        return forcing[d * n + i, j] if forced else 0.0

    def edges(i, _):
        p7, u7 = cur[0, i, :, last, :], cur[3, i, :, last, :]
        p0, u0 = cur[0, i, :, 0, :], cur[3, i, :, 0, :]
        plus, minus = u7 + p7, u0 - p0
        below = jnp.where(z == 0, turn(plus, 1 - EZ), turn(plus, 1))
        above = jnp.where(z == EZ - 1, turn(minus, EZ - 1), turn(minus, -1))
        edge[0, i] = lift * (below - (u0 + p0))
        edge[1, i] = lift * (above - (u7 - p7))
        return 0

    lax.fori_loop(0, n, edges, 0)

    def lines_i(j, _):
        d_u = derive([cur[1, i, j] for i in range(n)], even, odd)
        d_p = derive([cur[0, i, j] for i in range(n)], even, odd)
        for i in range(n):
            store(1, i, j, push(0, i, j) - d_p[i])
            rate_p, rate_w = d_u[i], 0.0
            for m in range(n):
                rate_p = rate_p + dcol[m] * cur[3, i, j, m : m + 1, :]
                rate_w = rate_w + dcol[m] * cur[0, i, j, m : m + 1, :]
            low = jnp.where(node == 0, edge[0, i, pl.ds(j, 1), :], 0.0)
            up = jnp.where(node == last, edge[1, i, pl.ds(j, 1), :], 0.0)
            partial[i, j] = (low - up) - rate_p
            store(3, i, j, push(2, i, j) + ((low + up) - rate_w))
        return 0

    lax.fori_loop(0, n, lines_i, 0)

    def lines_j(i, _):
        p = [cur[0, i, j] for j in range(n)]
        v = [cur[2, i, j] for j in range(n)]
        low = lift * (turn(v[last] + p[last], EZ) - (v[0] + p[0]))
        up = lift * (turn(v[0] - p[0], -EZ) - (v[last] - p[last]))
        d_v = derive(v, even, odd)
        d_p = derive(p, even, odd)
        for j in range(n):
            rate_p, rate_v = partial[i, j] - d_v[j], push(1, i, j) - d_p[j]
            if j == 0:
                rate_p, rate_v = rate_p + low, rate_v + low
            if j == last:
                rate_p, rate_v = rate_p - up, rate_v + up
            store(0, i, j, rate_p)
            store(2, i, j, rate_v)
        return 0

    lax.fori_loop(0, n, lines_j, 0)


def wave_force(out, forcing, stage):
    n = out.shape[1]
    scale = GAIN[stage] * ACOUSTIC_STEP

    def body(i, _):
        for d in range(3):
            out[1 + d, i] = out[1 + d, i] + scale * forcing[d * n + i]
        return 0

    lax.fori_loop(0, n, body, 0)


def wave_faces(cur, out, below, above, lift, stage):
    last = cur.shape[1] - 1
    scale = GAIN[stage] * ACOUSTIC_STEP * lift
    low = scale * (below[...] - (cur[1, 0] + cur[0, 0]))
    out[0, 0] = out[0, 0] + low
    out[1, 0] = out[1, 0] + low
    up = scale * (above[...] - (cur[1, last] - cur[0, last]))
    out[0, last] = out[0, last] - up
    out[1, last] = out[1, last] + up


def all_kernel(
    sizes, den_hbm, vel_hbm, pre_hbm, wave_hbm, tables_hbm, element, block, table,
    fields_out, wave_out, forcing_out,
    den, vel, pre, wave0, tables, high, low, X, YA, YB, S, pick, label, label_in, place,
    mapped_high, mapped_low, send, recv, forcing1, partial, edge, dcol, V, FS, FR,
    local_sem, x_send, x_recv, y_send, y_recv, w_send, w_recv, l_send, l_recv, a_send, a_recv,
):
    flows, groups, local_count = sizes
    devices = flows * groups
    planes, rows, columns = den.shape
    f, g = lax.axis_index("flow"), lax.axis_index("group")
    me = f * groups + g
    at = lambda k: (k // groups, k % groups)
    matrix, end_weight = lobatto(wave0.shape[1])
    lift = 0.5 / end_weight
    n = wave0.shape[1]

    loads = [
        pltpu.make_async_copy(a, b, local_sem.at[i])
        for i, (a, b) in enumerate(
            [(den_hbm, den), (vel_hbm, vel), (pre_hbm, pre), (wave_hbm, wave0), (tables_hbm, tables)]
        )
    ]
    for c in loads:
        c.start()
    barrier = pltpu.get_barrier_semaphore()

    def greet(d, _):
        pl.semaphore_signal(
            barrier, inc=1, device_id=at((me + d) % devices), device_id_type=pl.DeviceIdType.MESH
        )
        return 0

    lax.fori_loop(1, devices, greet, 0)

    pending = []

    def remote(src, dst, ssem, rsem, device):
        c = pltpu.make_async_remote_copy(
            src_ref=src, dst_ref=dst, send_sem=ssem, recv_sem=rsem,
            device_id=device, device_id_type=pl.DeviceIdType.MESH,
        )
        c.start()
        pending.append(c)
        return c

    def send_halos(s):
        own = slice(1, planes + 1)
        r8 = YA.shape[3]
        up_g, down_g = (g + 1) % groups, (g + groups - 1) % groups
        up_f, down_f = (f + 1) % flows, (f + flows - 1) % flows
        return [
            remote(X.at[s, :, 1], X.at[s, :, planes + 1], x_send.at[s, 0], x_recv.at[s, 0], (down_f, g)),
            remote(X.at[s, :, planes], X.at[s, :, 0], x_send.at[s, 1], x_recv.at[s, 1], (up_f, g)),
            remote(X.at[s, :, own, 0:r8], YA.at[s], y_send.at[s, 0], y_recv.at[s, 0], (f, down_g)),
            remote(X.at[s, :, own, rows - r8 :], YB.at[s], y_send.at[s, 1], y_recv.at[s, 1], (f, up_g)),
        ]

    def send_faces(s, cur):
        last = n - 1
        FS[s, 0] = cur[1, last] + cur[0, last]
        FS[s, 1] = cur[1, 0] - cur[0, 0]
        return [
            remote(FS.at[s, 0], FR.at[s, 0], w_send.at[s, 0], w_recv.at[s, 0], at((me + 1) % devices)),
            remote(FS.at[s, 1], FR.at[s, 1], w_send.at[s, 1], w_recv.at[s, 1], at((me + devices - 1) % devices)),
        ]

    def arrive(copies):
        for c in copies:
            c.wait_recv()

    high_rows = 2 * CAP

    def slot_copy(src, dst, ssem, rsem, peer, owner):
        block_at = lambda k: pl.ds(pl.multiple_of(k * high_rows, high_rows), high_rows)
        return pltpu.make_async_remote_copy(
            src_ref=src.at[block_at(peer)], dst_ref=dst.at[block_at(owner)],
            send_sem=ssem.at[peer], recv_sem=rsem.at[owner],
            device_id=at(peer), device_id_type=pl.DeviceIdType.MESH,
        )

    def exchange(src, dst, ssem, rsem, begin, end):
        def body(d, _):
            slot_copy(src, dst, ssem, rsem, (me + d) % devices, me).start()
            return 0
        lax.fori_loop(begin, end, body, 0)

    def keep_own(src, dst):
        mine = pl.ds(pl.multiple_of(me * high_rows, high_rows), high_rows)
        dst[mine, :] = src[mine, :]

    def settle(src, dst, ssem, rsem):
        def body(d, _):
            slot_copy(src, dst, ssem, rsem, (me + d) % devices, (me + d) % devices).wait_recv()
            return 0
        lax.fori_loop(1, devices, body, 0)

    def drain(src, dst, ssem, rsem):
        def body(d, _):
            slot_copy(src, dst, ssem, rsem, (me + d) % devices, (me + d) % devices).wait_send()
            return 0
        lax.fori_loop(1, devices, body, 0)

    for c in loads[:3]:
        c.wait()

    def conserve(p, _):
        r = den[p]
        v = [vel[d, p] for d in range(3)]
        X[0, 0, p + 1] = r
        for d in range(3):
            X[0, 1 + d, p + 1] = r * v[d]
        square = v[0] * v[0] + v[1] * v[1] + v[2] * v[2]
        X[0, 4, p + 1] = pre[p] / (GAMMA - 1.0) + 0.5 * r * square
        return 0

    lax.fori_loop(0, planes, conserve, 0)
    pl.semaphore_wait(barrier, devices - 1)
    halo = send_halos(0)
    loads[3].wait()
    waves = send_faces(0, wave0)
    blocks = planes * rows * columns // tables.shape[1]
    routes(element[...], block[...], table[...], blocks, tables.shape[0], local_count, devices, pick, label)
    exchange(label, label_in, l_send, l_recv, 1, devices)
    keep_own(label, label_in)
    row = iota((n, dcol.shape[-1]), 0)
    for m in range(n):
        tile = jnp.zeros((n, dcol.shape[-1]), F32)
        for k in range(n):
            tile = jnp.where(row == k, float(matrix[k, m]), tile)
        dcol[m] = tile
    loads[4].wait()
    split_tables(tables, high, low)

    forcings = [forcing1, forcing_out]
    cuts = [1, 1 + (devices - 1) // 3, 1 + 2 * (devices - 1) // 3, devices]

    def flow_part(s):
        step, stage = s // 3, s % 3
        base = 3 * step

        def finish(p, c, value):
            if stage:
                value = KEEP[stage] * X[base, c, p + 1] + GAIN[stage] * value
            if s == 3 * STEPS - 1:
                fields_out[c, p] = value
            else:
                X[s + 1, c, p + 1] = value

        flow_stage(X.at[s], YA.at[s], YB.at[s], finish)

    def project(step):
        rows_of_slots(S, high, low, pick, mapped_high, mapped_low, send.at[step])
        keep_own(send.at[step], recv.at[step])

    def issue(step, part):
        exchange(send.at[step], recv.at[step], a_send.at[step], a_recv.at[step], cuts[part], cuts[part + 1])

    curs = [wave0] + [V.at[i] for i in range(5)] + [wave_out]

    def main(s, forced):
        step, stage = s // 3, s % 3
        wave_main(curs[3 * step], curs[s], forcings[step], curs[s + 1], partial, edge, dcol,
                  matrix, lift, stage, forced)

    def finish_wave(s, copies):
        arrive(copies)
        wave_faces(curs[s], curs[s + 1], FR.at[s, 0], FR.at[s, 1], lift, s % 3)

    main(0, False)
    arrive(halo)
    flow_part(0)
    halo = send_halos(1)
    lamb(X.at[0], YA.at[0], YB.at[0], S)
    project(0)
    issue(0, 0)
    arrive(halo)
    flow_part(1)
    halo = send_halos(2)
    issue(0, 1)
    arrive(halo)
    flow_part(2)
    halo = send_halos(3)
    issue(0, 2)
    settle(label, label_in, l_send, l_recv)
    place_of(label_in, place)
    arrive(halo)
    flow_part(3)
    halo = send_halos(4)
    lamb(X.at[3], YA.at[3], YB.at[3], S)
    project(1)
    settle(send.at[0], recv.at[0], a_send.at[0], a_recv.at[0])
    add_up(recv.at[0], place, forcing1)
    finish_wave(0, waves)
    wave_force(curs[1], forcing1, 0)
    waves = send_faces(1, curs[1])
    issue(1, 0)
    main(1, True)
    arrive(halo)
    flow_part(4)
    halo = send_halos(5)
    finish_wave(1, waves)
    waves = send_faces(2, curs[2])
    issue(1, 1)
    main(2, True)
    finish_wave(2, waves)
    waves = send_faces(3, curs[3])
    issue(1, 2)
    main(3, False)
    arrive(halo)
    flow_part(5)
    settle(send.at[1], recv.at[1], a_send.at[1], a_recv.at[1])
    add_up(recv.at[1], place, forcing_out)
    finish_wave(3, waves)
    wave_force(curs[4], forcing_out, 0)
    waves = send_faces(4, curs[4])
    main(4, True)
    finish_wave(4, waves)
    waves = send_faces(5, curs[5])
    main(5, True)
    finish_wave(5, waves)
    for c in pending:
        c.wait_send()
    drain(label, label_in, l_send, l_recv)
    for step in range(STEPS):
        drain(send.at[step], recv.at[step], a_send.at[step], a_recv.at[step])


def local(
    density, velocity, pressure, wave_state, tables, margin_element, margin_block, margin_table
):
    flows, groups = lax.axis_size("flow"), lax.axis_size("group")
    devices = flows * groups
    planes, rows, columns = density.shape
    n, lanes = wave_state.shape[1], wave_state.shape[-1]
    table_count, depth, nodes = tables.shape
    blocks = density.size // depth
    lines = devices * 2 * CAP
    half = 3 * nodes // 2
    cols = 2 * table_count * blocks
    stages = 3 * STEPS
    side = 8
    any_spec = pl.BlockSpec(memory_space=pl.ANY)
    vmem = pl.BlockSpec(memory_space=pltpu.VMEM)
    V = pltpu.VMEM
    DMA = pltpu.SemaphoreType.DMA
    wave_shape = wave_state.shape

    def body(*refs):
        all_kernel((flows, groups, lanes), *refs)

    fields, wave, forcing = pl.pallas_call(
        body,
        out_shape=(
            jax.ShapeDtypeStruct((5, planes, rows, columns), F32),
            jax.ShapeDtypeStruct(wave_shape, F32),
            jax.ShapeDtypeStruct((3 * n, n, n, lanes), F32),
        ),
        in_specs=[any_spec] * 5 + [vmem] * 3,
        out_specs=(vmem, vmem, vmem),
        scratch_shapes=[
            V((planes, rows, columns), F32), V((3, planes, rows, columns), F32),
            V((planes, rows, columns), F32), V(wave_shape, F32), V(tables.shape, F32),
            V(tables.shape, BF16), V(tables.shape, BF16),
            V((stages, 5, planes + 2, rows, columns), F32),
            V((stages, 5, planes, side, columns), F32), V((stages, 5, planes, side, columns), F32),
            V((3, planes, columns // 128, rows, 128), F32),
            V((lines, cols), BF16), V((lines, lanes), jnp.int32), V((lines, lanes), jnp.int32),
            V((lines, 2 * lanes), BF16),
            V((cols, half), BF16), V((cols, half), BF16),
            V((STEPS, lines, half), F32), V((STEPS, lines, half), F32),
            V((3 * n, n, n, lanes), F32),
            V((n, n, n, lanes), F32), V((2, n, n, lanes), F32), V((n, n, lanes), F32),
            V((5,) + wave_shape, F32),
            V((stages, 2, n, n, lanes), F32), V((stages, 2, n, n, lanes), F32),
            DMA((5,)), DMA((stages, 2)), DMA((stages, 2)), DMA((stages, 2)), DMA((stages, 2)),
            DMA((stages, 2)), DMA((stages, 2)), DMA((devices,)), DMA((devices,)),
            DMA((STEPS, devices)), DMA((STEPS, devices)),
        ],
        compiler_params=pltpu.CompilerParams(
            collective_id=0, has_side_effects=True, vmem_limit_bytes=60000 * 1024
        ),
        name="march",
    )(density, velocity, pressure, wave_state, tables, margin_element, margin_block, margin_table)
    return fields, wave, forcing.reshape((3, n, n, n, lanes))


def solution(mesh):
    in_specs = (
        P("flow", "group", None),
        P(None, "flow", "group", None),
        P("flow", "group", None),
        P(None, None, None, None, ("flow", "group")),
        P(),
        P(("flow", "group"), None),
        P(("flow", "group"), None),
        P(("flow", "group"), None),
    )
    out_specs = (
        P(None, "flow", "group", None),
        P(None, None, None, None, ("flow", "group")),
        P(None, None, None, None, ("flow", "group")),
    )
    return jax.shard_map(local, mesh=mesh, in_specs=in_specs, out_specs=out_specs, check_vma=False)
```

```python
import jax
import jax.numpy as jnp
import numpy as np
from jax import lax
from jax.experimental import pallas as pl
from jax.experimental.pallas import tpu as pltpu
from jax.sharding import PartitionSpec as P

EZ = 16
CAP = 4
STEPS = 2

GAMMA = 1.4
DT_FLOW = 0.08
ACOUSTIC_STEP = 0.01
F32, BF16 = jnp.float32, jnp.bfloat16
KEEP = (0.0, 0.75, 1.0 / 3.0)
GAIN = (1.0, 0.25, 2.0 / 3.0)


def legendre_pair(quadrature_nodes, degree):
    previous = np.ones(quadrature_nodes.shape[0])
    current = quadrature_nodes * 1.0
    for order in range(2, degree + 1):
        previous, current = (
            current,
            ((2 * order - 1) * quadrature_nodes * current - (order - 1) * previous) / order,
        )
    return (previous, current)


def lobatto(point_count):
    degree = point_count - 1
    quadrature_nodes = -np.cos(np.pi * np.arange(point_count) / degree)
    for sweep in range(60):
        previous, current = legendre_pair(quadrature_nodes, degree)
        quadrature_nodes = quadrature_nodes - (quadrature_nodes * current - previous) / (
            point_count * current
        )
    previous, values = legendre_pair(quadrature_nodes, degree)
    quadrature_weights = 2.0 / (degree * (degree + 1) * values**2)
    identity = np.eye(point_count)
    differ = quadrature_nodes[:, None] - quadrature_nodes[None, :] + identity
    matrix = values[:, None] / values[None, :] / differ * (1.0 - identity)
    matrix[0, 0] = -degree * (degree + 1) / 4.0
    matrix[-1, -1] = degree * (degree + 1) / 4.0
    return (matrix, float(quadrature_weights[0]))


def iota(shape, axis):
    return lax.broadcasted_iota(jnp.int32, shape, axis)


def split(value):
    high = value.astype(BF16)
    return high, (value - high.astype(F32)).astype(BF16)


def dot(a, b):
    return jnp.dot(a, b, preferred_element_type=F32)


def primitive(state):
    inverse = 1.0 / state[0]
    vel = [state[1 + d] * inverse for d in range(3)]
    square = vel[0] * vel[0] + vel[1] * vel[1] + vel[2] * vel[2]
    pressure = (GAMMA - 1.0) * (state[4] - 0.5 * state[0] * square)
    return vel, pressure, jnp.sqrt(GAMMA * pressure * inverse)


def flux_of(state, prim, d):
    vel, pressure, sound = prim
    normal = vel[d]
    parts = [state[0] * normal]
    for c in range(3):
        product = state[1 + c] * normal
        parts.append(product + pressure if c == d else product)
    parts.append((state[4] + pressure) * normal)
    return parts, jnp.abs(normal) + sound


def face(left, right, left_flux, right_flux, left_speed, right_speed):
    speed = jnp.maximum(left_speed, right_speed)
    return [
        0.5 * (left_flux[c] + right_flux[c]) - 0.5 * speed * (right[c] - left[c])
        for c in range(5)
    ]


def along(cell, prim, d, axis):
    size = cell[0].shape[axis]
    flux, speed = flux_of(cell, prim, d)
    back = lambda v: pltpu.roll(v, size - 1, axis)
    upper = face(
        cell, [back(v) for v in cell], flux, [back(v) for v in flux], speed, back(speed)
    )
    return [upper[c] - pltpu.roll(upper[c], 1, axis) for c in range(5)]


def tall_of(own, above, below):
    row = iota(above.shape, 0)
    return jnp.concatenate([own, jnp.where(row < above.shape[0] // 2, above, below)], axis=0)


def flow_stage(src, above, below, finish, before, after):
    planes, rows = src.shape[1] - 2, src.shape[2]

    def load(p):
        return [src[c, p] for c in range(5)]

    def x_side(p):
        cell = load(p)
        flux, speed = flux_of(cell, primitive(cell), 0)
        return cell, flux, speed

    def x_face(p):
        left, right = x_side(p), x_side(p + 1)
        return face(left[0], right[0], left[1], right[1], left[2], right[2])

    def body(p, lower):
        before(p)
        upper = x_face(p + 1)
        tall = [tall_of(src[c, p + 1], above[c, p], below[c, p]) for c in range(5)]
        prim = primitive(tall)
        dy = along(tall, prim, 1, 0)
        cell = [v[:rows] for v in tall]
        prim = ([v[:rows] for v in prim[0]], prim[1][:rows], prim[2][:rows])
        dz = along(cell, prim, 2, 1)
        for c in range(5):
            rate = -(upper[c] - lower[c]) - dy[c][:rows] - dz[c]
            finish(p, c, cell[c] + DT_FLOW * rate)
        after(p)
        return tuple(upper)

    lax.fori_loop(0, planes, body, tuple(x_face(0)))


def lamb(src, above, below, out):
    planes, rows, columns = src.shape[1] - 2, src.shape[2], src.shape[3]

    def body(p, _):
        density = tall_of(src[0, p + 1], above[0, p], below[0, p])
        inverse = 1.0 / density
        tall = [
            tall_of(src[1 + d, p + 1], above[1 + d, p], below[1 + d, p]) * inverse
            for d in range(3)
        ]
        size = tall[0].shape[0]
        slope_y = [
            0.5 * (pltpu.roll(v, size - 1, 0) - pltpu.roll(v, 1, 0))[:rows] for v in tall
        ]
        vel = [v[:rows] for v in tall]
        slope_z = [0.5 * (pltpu.roll(v, columns - 1, 1) - pltpu.roll(v, 1, 1)) for v in vel]
        after, before = 1.0 / src[0, p + 2], 1.0 / src[0, p]
        slope_x = [
            0.5 * (src[1 + d, p + 2] * after - src[1 + d, p] * before) for d in range(3)
        ]
        curl_x = slope_y[2] - slope_z[1]
        curl_y = slope_z[0] - slope_x[2]
        curl_z = slope_x[1] - slope_y[0]
        result = [
            curl_y * vel[2] - curl_z * vel[1],
            curl_z * vel[0] - curl_x * vel[2],
            curl_x * vel[1] - curl_y * vel[0],
        ]
        for d in range(3):
            for q in range(out.shape[2]):
                out[d, p, q] = result[d][:, q * 128 : (q + 1) * 128]
        return 0

    lax.fori_loop(0, planes, body, 0)


def split_tables(tables, high, low):
    count, depth, _ = tables.shape
    step = 64

    def body(i, _):
        t = i // (depth // step)
        at = pl.ds(pl.multiple_of((i % (depth // step)) * step, step), step)
        h, l = split(tables[t, at, :])
        high[t, at, :] = h
        low[t, at, :] = l
        return 0

    lax.fori_loop(0, count * (depth // step), body, 0)


def rows_of_slots(source, high, low, pick, mapped_high, mapped_low, send):
    _, planes, chunks, rows, width = source.shape
    columns = chunks * width
    table_count, depth, nodes = high.shape
    per = depth // columns
    strip = rows // per
    blocks = planes * strip
    half = 3 * nodes // 2
    pieces = []
    for y in range(3):
        for p in range(planes):
            pieces.append(
                jnp.concatenate(
                    [
                        source[y, p, q, pl.ds(r, strip, stride=per), :]
                        for r in range(per)
                        for q in range(chunks)
                    ],
                    axis=1,
                )
            )
    left_high, left_low = split(jnp.concatenate(pieces, axis=0))
    both = jnp.concatenate([left_high, left_low], axis=0)
    count = 3 * blocks

    def body(t, _):
        wide = dot(both, high[t])
        out = wide[:count] + wide[count:] + dot(left_high, low[t])
        for side in range(2):
            at = pl.ds(pl.multiple_of(side * table_count * blocks + t * blocks, blocks), blocks)
            for y in range(3):
                begin, end = max(y * nodes, side * half), min((y + 1) * nodes, (side + 1) * half)
                if begin < end:
                    value = out[y * blocks : (y + 1) * blocks, begin - y * nodes : end - y * nodes]
                    h, l = split(value)
                    mapped_high[at, begin - side * half : end - side * half] = h
                    mapped_low[at, begin - side * half : end - side * half] = l
        return 0

    lax.fori_loop(0, table_count, body, 0)
    send[...] = dot(pick[...], mapped_high[...]) + dot(pick[...], mapped_low[...])


def routes(element, block, table, blocks, table_count, local_count, devices, pick, label):
    entries = element.shape[1]
    shift = local_count.bit_length() - 1
    assert 1 << shift == local_count
    owner = lax.shift_right_logical(element, shift)
    local_index = element - lax.shift_left(owner, shift)
    column = table * blocks + block
    square = (entries, entries)
    row = jnp.broadcast_to(owner, square)
    turned = jnp.sum(jnp.where(iota(square, 0) == iota(square, 1), row, 0), axis=1, keepdims=True)
    earlier = (turned == row) & (iota(square, 0) < iota(square, 1))
    rank = jnp.sum(jnp.where(earlier, 1, 0), axis=0, keepdims=True)
    slot = owner * CAP + rank
    high = 2 * CAP
    lines = devices * high
    line = iota((lines, entries), 0)
    named = (line // high) * CAP + line % CAP
    hit = named == slot
    labels = jnp.sum(jnp.where(hit, local_index + 1, 0), axis=1, keepdims=True) - 1
    picked = jnp.sum(jnp.where(hit, column + 1, 0), axis=1, keepdims=True) - 1
    tiles = (devices, high, label.shape[2])
    spread = jnp.broadcast_to(labels, (lines, tiles[2])).reshape(tiles)
    label[...] = jnp.sum(
        jnp.where(iota(tiles, 1) == iota(tiles, 2), spread, 0), axis=1, keepdims=True
    )
    shape = pick.shape
    side = (iota(shape, 0) // CAP) % 2
    chosen = picked + side * (table_count * blocks)
    on = (iota(shape, 1) == chosen) & (picked >= 0)
    pick[...] = jnp.where(on, 1.0, 0.0).astype(BF16)


def place_of(label, place):
    devices, _, lanes = label.shape
    high = 2 * CAP
    shape = (devices * high, lanes)
    wide = jnp.broadcast_to(label[...], (devices, high, lanes)).reshape(shape)
    line, lane = iota(shape, 0), iota(shape, 1)
    named = jnp.sum(jnp.where(line % CAP == lane, wide, 0), axis=1, keepdims=True)
    side = (line // CAP) % 2
    hit = named == lane
    for s in range(2):
        place[:, s * lanes : (s + 1) * lanes] = jnp.where(hit & (side == s), 1.0, 0.0).astype(BF16)


def add_up(received, place, forcing):
    parts, lanes = forcing.shape[0] // 2, forcing.shape[-1]
    high, low = split(received[...].T)
    total = dot(high, place[...]) + dot(low, place[...])
    for s in range(2):
        forcing[s * parts : (s + 1) * parts] = total[:, s * lanes : (s + 1) * lanes].reshape(
            (parts,) + forcing.shape[1:]
        )


def halves(matrix):
    n = matrix.shape[0]
    turned = matrix[: n // 2, ::-1][:, : n // 2]
    own = matrix[: n // 2, : n // 2]
    return 0.5 * (own + turned), 0.5 * (own - turned)


def derive(values, even, odd):
    n = len(values)
    h = n // 2
    sums = [values[m] + values[n - 1 - m] for m in range(h)]
    gaps = [values[m] - values[n - 1 - m] for m in range(h)]
    out = [None] * n
    for a in range(h):
        alpha = sum(float(even[a, m]) * sums[m] for m in range(h))
        beta = sum(float(odd[a, m]) * gaps[m] for m in range(h))
        out[a] = beta + alpha
        out[n - 1 - a] = beta - alpha
    return out


def wave_main(start, cur, forcing, out, partial, edge, dcol, matrix, lift, stage, forced):
    keep, gain = KEEP[stage], GAIN[stage]
    n, lanes = cur.shape[1], cur.shape[-1]
    last = n - 1
    even, odd = halves(matrix)
    node = iota((n, lanes), 0)
    z = iota((n, lanes), 1) % EZ
    turn = lambda v, by: pltpu.roll(v, by % lanes, v.ndim - 1)

    def store(f, i, j, rate):
        value = gain * cur[f, i, j] + (gain * ACOUSTIC_STEP) * rate
        if keep:
            value = keep * start[f, i, j] + value
        out[f, i, j] = value

    def push(d, i, j):
        return forcing[d * n + i, j] if forced else 0.0

    def edges(i, _):
        p7, u7 = cur[0, i, :, last, :], cur[3, i, :, last, :]
        p0, u0 = cur[0, i, :, 0, :], cur[3, i, :, 0, :]
        plus, minus = u7 + p7, u0 - p0
        below = jnp.where(z == 0, turn(plus, 1 - EZ), turn(plus, 1))
        above = jnp.where(z == EZ - 1, turn(minus, EZ - 1), turn(minus, -1))
        edge[0, i] = lift * (below - (u0 + p0))
        edge[1, i] = lift * (above - (u7 - p7))
        return 0

    lax.fori_loop(0, n, edges, 0)

    def lines_i(j, _):
        d_u = derive([cur[1, i, j] for i in range(n)], even, odd)
        d_p = derive([cur[0, i, j] for i in range(n)], even, odd)
        for i in range(n):
            store(1, i, j, push(0, i, j) - d_p[i])
            rate_p, rate_w = d_u[i], 0.0
            for m in range(n):
                rate_p = rate_p + dcol[m] * cur[3, i, j, m : m + 1, :]
                rate_w = rate_w + dcol[m] * cur[0, i, j, m : m + 1, :]
            low = jnp.where(node == 0, edge[0, i, pl.ds(j, 1), :], 0.0)
            up = jnp.where(node == last, edge[1, i, pl.ds(j, 1), :], 0.0)
            partial[i, j] = (low - up) - rate_p
            store(3, i, j, push(2, i, j) + ((low + up) - rate_w))
        return 0

    lax.fori_loop(0, n, lines_i, 0)

    def lines_j(i, _):
        p = [cur[0, i, j] for j in range(n)]
        v = [cur[2, i, j] for j in range(n)]
        low = lift * (turn(v[last] + p[last], EZ) - (v[0] + p[0]))
        up = lift * (turn(v[0] - p[0], -EZ) - (v[last] - p[last]))
        d_v = derive(v, even, odd)
        d_p = derive(p, even, odd)
        for j in range(n):
            rate_p, rate_v = partial[i, j] - d_v[j], push(1, i, j) - d_p[j]
            if j == 0:
                rate_p, rate_v = rate_p + low, rate_v + low
            if j == last:
                rate_p, rate_v = rate_p - up, rate_v + up
            store(0, i, j, rate_p)
            store(2, i, j, rate_v)
        return 0

    lax.fori_loop(0, n, lines_j, 0)


def wave_force(out, forcing, stage):
    n = out.shape[1]
    scale = GAIN[stage] * ACOUSTIC_STEP

    def body(i, _):
        for d in range(3):
            out[1 + d, i] = out[1 + d, i] + scale * forcing[d * n + i]
        return 0

    lax.fori_loop(0, n, body, 0)


def wave_faces(cur, out, below, above, lift, stage):
    last = cur.shape[1] - 1
    scale = GAIN[stage] * ACOUSTIC_STEP * lift
    low = scale * (below[...] - (cur[1, 0] + cur[0, 0]))
    out[0, 0] = out[0, 0] + low
    out[1, 0] = out[1, 0] + low
    up = scale * (above[...] - (cur[1, last] - cur[0, last]))
    out[0, last] = out[0, last] - up
    out[1, last] = out[1, last] + up


def all_kernel(
    sizes, den_hbm, vel_hbm, pre_hbm, wave_hbm, tables_hbm, element, block, table,
    fields_out, wave_out, forcing_out,
    den, vel, pre, wave0, tables, high, low, X0, X1, X2, X3, X4, X5,
    A0, A1, A2, A3, A4, A5, B0, B1, B2, B3, B4, B5, S, pick, label, label_in, place,
    mapped_high, mapped_low, send, recv, forcing1, partial, edge, dcol, V, FS, FR,
    local_sem, x_send, x_recv, y_send, y_recv, w_send, w_recv, l_send, l_recv, a_send, a_recv,
):
    flows, groups, local_count = sizes
    devices = flows * groups
    planes, rows, columns = den.shape
    f, g = lax.axis_index("flow"), lax.axis_index("group")
    me = f * groups + g
    at = lambda k: (k // groups, k % groups)
    matrix, end_weight = lobatto(wave0.shape[1])
    lift = 0.5 / end_weight
    n = wave0.shape[1]

    loads = [
        pltpu.make_async_copy(a, b, local_sem.at[i])
        for i, (a, b) in enumerate(
            [(den_hbm, den), (vel_hbm, vel), (pre_hbm, pre), (wave_hbm, wave0), (tables_hbm, tables)]
        )
    ]
    for c in loads:
        c.start()
    barrier = pltpu.get_barrier_semaphore()

    def greet(d, _):
        pl.semaphore_signal(
            barrier, inc=1, device_id=at((me + d) % devices), device_id_type=pl.DeviceIdType.MESH
        )
        return 0

    lax.fori_loop(1, devices, greet, 0)

    pending = []

    def remote(src, dst, ssem, rsem, device):
        c = pltpu.make_async_remote_copy(
            src_ref=src, dst_ref=dst, send_sem=ssem, recv_sem=rsem,
            device_id=device, device_id_type=pl.DeviceIdType.MESH,
        )
        c.start()
        pending.append(c)
        return c

    X = [X0, X1, X2, X3, X4, X5]
    A, B = [A0, A1, A2, A3, A4, A5], [B0, B1, B2, B3, B4, B5]
    r8 = A0.shape[2]
    up_g, down_g = (f, (g + 1) % groups), (f, (g + groups - 1) % groups)
    up_f, down_f = ((f + 1) % flows, g), ((f + flows - 1) % flows, g)

    def y_copies(s, p):
        return [
            pltpu.make_async_remote_copy(
                src_ref=X[s].at[:, p + 1, band], dst_ref=ghost[s].at[:, p],
                send_sem=y_send.at[s, way, p], recv_sem=y_recv.at[s, way, p],
                device_id=device, device_id_type=pl.DeviceIdType.MESH,
            )
            for way, (band, ghost, device) in enumerate(
                [(slice(0, r8), A, down_g), (slice(rows - r8, rows), B, up_g)]
            )
        ]

    def send_y(s, p):
        for c in y_copies(s, p):
            c.start()

    def wait_y(s, p):
        for c in y_copies(s, p):
            c.wait_recv()

    def over(begin, end, do):
        def body(p, _):
            do(p)
            return 0
        lax.fori_loop(begin, end, body, 0)

    def send_x(s, i, low, low_to, high, high_to):
        return [
            remote(X[s].at[:, low], X[s].at[:, low_to], x_send.at[s, i], x_recv.at[s, i], down_f),
            remote(X[s].at[:, high], X[s].at[:, high_to], x_send.at[s, i + 1], x_recv.at[s, i + 1], up_f),
        ]

    def send_halos(s):
        return send_x(s, 0, slice(1, 2), slice(planes + 1, planes + 2), slice(planes, planes + 1), slice(0, 1))

    def send_faces(s, cur):
        last = n - 1
        FS[s, 0] = cur[1, last] + cur[0, last]
        FS[s, 1] = cur[1, 0] - cur[0, 0]
        return [
            remote(FS.at[s, 0], FR.at[s, 0], w_send.at[s, 0], w_recv.at[s, 0], at((me + 1) % devices)),
            remote(FS.at[s, 1], FR.at[s, 1], w_send.at[s, 1], w_recv.at[s, 1], at((me + devices - 1) % devices)),
        ]

    def arrive(copies):
        for c in copies:
            c.wait_recv()

    high_rows = 2 * CAP

    def slot_copy(src, dst, ssem, rsem, peer, owner):
        size = src.shape[0] // devices
        block_at = lambda k: pl.ds(pl.multiple_of(k * size, size), size)
        return pltpu.make_async_remote_copy(
            src_ref=src.at[block_at(peer)], dst_ref=dst.at[block_at(owner)],
            send_sem=ssem, recv_sem=rsem,
            device_id=at(peer), device_id_type=pl.DeviceIdType.MESH,
        )

    stride = 11 if np.gcd(11, devices) == 1 else 1

    def exchange(src, dst, ssem, rsem, begin, end):
        def body(k, _):
            slot_copy(src, dst, ssem, rsem, (me + k * stride) % devices, me).start()
            return 0
        lax.fori_loop(begin, end, body, 0)

    def keep_own(src, dst):
        size = src.shape[0] // devices
        mine = pl.ds(pl.multiple_of(me * size, size), size)
        dst[mine] = src[mine]

    def all_blocks(src, dst, ssem, rsem):
        others = pl.ds(0, (devices - 1) * (src.shape[0] // devices))
        return pltpu.make_async_remote_copy(
            src_ref=src.at[others], dst_ref=dst.at[others], send_sem=ssem, recv_sem=rsem,
            device_id=at((me + 1) % devices), device_id_type=pl.DeviceIdType.MESH,
        )

    def settle(*refs):
        all_blocks(*refs).wait_recv()

    def drain(*refs):
        all_blocks(*refs).wait_send()

    for c in loads[:3]:
        c.wait()

    deep = 4
    assert planes >= deep

    def conserve(p, _):
        r = den[p]
        v = [vel[d, p] for d in range(3)]
        X0[0, p + deep] = r
        for d in range(3):
            X0[1 + d, p + deep] = r * v[d]
        square = v[0] * v[0] + v[1] * v[1] + v[2] * v[2]
        X0[4, p + deep] = pre[p] / (GAMMA - 1.0) + 0.5 * r * square
        return 0

    lax.fori_loop(0, planes, conserve, 0)
    pl.semaphore_wait(barrier, devices - 1)
    near = send_x(
        0, 0, slice(deep, deep + 1), slice(deep + planes, deep + planes + 1),
        slice(deep + planes - 1, deep + planes), slice(deep - 1, deep),
    )
    over(deep - 1, deep - 1 + planes, lambda p: send_y(0, p))
    far = send_x(
        0, 2, slice(deep + 1, 2 * deep), slice(deep + planes + 1, 2 * deep + planes),
        slice(planes, deep + planes - 1), slice(0, deep - 1),
    )
    loads[3].wait()
    waves = send_faces(0, wave0)
    blocks = planes * rows * columns // tables.shape[1]
    routes(element[...], block[...], table[...], blocks, tables.shape[0], local_count, devices, pick, label)
    exchange(label, label_in, l_send, l_recv, 1, devices)
    keep_own(label, label_in)
    row = iota((n, dcol.shape[-1]), 0)
    for m in range(n):
        tile = jnp.zeros((n, dcol.shape[-1]), F32)
        for k in range(n):
            tile = jnp.where(row == k, float(matrix[k, m]), tile)
        dcol[m] = tile
    loads[4].wait()
    split_tables(tables, high, low)

    forcings = [forcing1, forcing_out]
    def flow_part(s):
        step, stage = s // 3, s % 3
        base = 3 * step
        lag = 1 if s >= 3 else 0
        total = X[s].shape[1] - 2

        def finish(p, c, value):
            if stage:
                value = KEEP[stage] * X[base][c, p + (stage + 1 if s < 3 else 1)] + GAIN[stage] * value
            if s == 3 * STEPS - 1:
                fields_out[c, p] = value
            else:
                X[s + 1][c, p + lag] = value

        def before(p):
            if s not in (0, 3):
                wait_y(s, p)

        def after(p):
            if s == 3 * STEPS - 1:
                return
            first = 1 if lag else 2

            @pl.when((p >= first) & (p - first < X[s + 1].shape[1] - 2))
            def _():
                send_y(s + 1, p - first)

        flow_stage(X[s], A[s], B[s], finish, before, after)
        if lag and s < 3 * STEPS - 1:
            send_y(s + 1, total - 1)

    def project(step):
        rows_of_slots(S, high, low, pick, mapped_high, mapped_low, send.at[step])
        keep_own(send.at[step], recv.at[step])

    def issue(step, begin, end):
        cut = lambda t: 1 + int(round(t * (devices - 1)))
        exchange(send.at[step], recv.at[step], a_send.at[step], a_recv.at[step], cut(begin), cut(end))

    curs = [wave0] + [V.at[i] for i in range(5)] + [wave_out]

    def main(s, forced):
        step, stage = s // 3, s % 3
        wave_main(curs[3 * step], curs[s], forcings[step], curs[s + 1], partial, edge, dcol,
                  matrix, lift, stage, forced)

    def finish_wave(s, copies):
        arrive(copies)
        wave_faces(curs[s], curs[s + 1], FR.at[s, 0], FR.at[s, 1], lift, s % 3)

    main(0, False)
    arrive(near)
    over(deep - 1, deep - 1 + planes, lambda p: wait_y(0, p))
    mid, own = pl.ds(deep - 1, planes + 2), pl.ds(deep - 1, planes)
    lamb(X0.at[:, mid], A0.at[:, own], B0.at[:, own], S)
    project(0)
    issue(0, 0.0, 1.0)
    arrive(far)
    for part in ((0, deep - 1), (deep - 1 + planes, 2 * deep + planes - 2)):
        over(*part, lambda p: send_y(0, p))
    for part in ((0, deep - 1), (deep - 1 + planes, 2 * deep + planes - 2)):
        over(*part, lambda p: wait_y(0, p))
    flow_part(0)
    flow_part(1)
    flow_part(2)
    over(0, planes, lambda p: wait_y(3, p))
    flow_part(3)
    halo = send_halos(4)
    lamb(X3, A3, B3, S)
    project(1)
    issue(1, 0.0, 0.1)
    settle(label, label_in, l_send, l_recv)
    place_of(label_in, place)
    settle(send.at[0], recv.at[0], a_send.at[0], a_recv.at[0])
    add_up(recv.at[0], place, forcing1)
    finish_wave(0, waves)
    wave_force(curs[1], forcing1, 0)
    waves = send_faces(1, curs[1])
    issue(1, 0.1, 0.4)
    main(1, True)
    finish_wave(1, waves)
    waves = send_faces(2, curs[2])
    arrive(halo)
    flow_part(4)
    halo = send_halos(5)
    issue(1, 0.4, 0.7)
    main(2, True)
    finish_wave(2, waves)
    waves = send_faces(3, curs[3])
    issue(1, 0.7, 1.0)
    main(3, False)
    arrive(halo)
    flow_part(5)
    for s in range(3 * STEPS):
        def drained(p, s=s):
            for c in y_copies(s, p):
                c.wait_send()
        over(0, X[s].shape[1] - 2, drained)
    drain(label, label_in, l_send, l_recv)
    drain(send.at[0], recv.at[0], a_send.at[0], a_recv.at[0])
    settle(send.at[1], recv.at[1], a_send.at[1], a_recv.at[1])
    add_up(recv.at[1], place, forcing_out)
    finish_wave(3, waves)
    wave_force(curs[4], forcing_out, 0)
    waves = send_faces(4, curs[4])
    main(4, True)
    finish_wave(4, waves)
    waves = send_faces(5, curs[5])
    main(5, True)
    drain(send.at[1], recv.at[1], a_send.at[1], a_recv.at[1])
    finish_wave(5, waves)
    for c in pending:
        c.wait_send()


def put_out(*values):
    count = len(values)

    def body(*refs):
        copies = [
            pltpu.make_async_copy(refs[i], refs[count + i], refs[2 * count].at[i])
            for i in range(count)
        ]
        for c in copies:
            c.start()
        for c in copies:
            c.wait()

    return pl.pallas_call(
        body,
        out_shape=tuple(jax.ShapeDtypeStruct(v.shape, v.dtype) for v in values),
        in_specs=[pl.BlockSpec(memory_space=pltpu.VMEM)] * count,
        out_specs=tuple([pl.BlockSpec(memory_space=pl.ANY)] * count),
        scratch_shapes=[pltpu.SemaphoreType.DMA((count,))],
        name="put_out",
    )(*[pltpu.with_memory_space_constraint(v, pltpu.VMEM) for v in values])


def local(
    density, velocity, pressure, wave_state, tables, margin_element, margin_block, margin_table
):
    flows, groups = lax.axis_size("flow"), lax.axis_size("group")
    devices = flows * groups
    planes, rows, columns = density.shape
    n, lanes = wave_state.shape[1], wave_state.shape[-1]
    table_count, depth, nodes = tables.shape
    blocks = density.size // depth
    lines = devices * 2 * CAP
    half = 3 * nodes // 2
    cols = 2 * table_count * blocks
    stages = 3 * STEPS
    side = 8
    widths = (8, 6, 4, 2, 2, 2)
    any_spec = pl.BlockSpec(memory_space=pltpu.HBM)
    vmem = pl.BlockSpec(memory_space=pltpu.VMEM)
    V = pltpu.VMEM
    DMA = pltpu.SemaphoreType.DMA
    wave_shape = wave_state.shape

    def body(*refs):
        all_kernel((flows, groups, lanes), *refs)

    fields, wave, forcing = pl.pallas_call(
        body,
        out_shape=(
            V((5, planes, rows, columns), F32),
            V(wave_shape, F32),
            V((3 * n, n, n, lanes), F32),
        ),
        in_specs=[any_spec] * 5 + [vmem] * 3,
        out_specs=(vmem, vmem, vmem),
        scratch_shapes=[
            V((planes, rows, columns), F32), V((3, planes, rows, columns), F32),
            V((planes, rows, columns), F32), V(wave_shape, F32), V(tables.shape, F32),
            V(tables.shape, BF16), V(tables.shape, BF16),
            *[V((5, planes + w, rows, columns), F32) for w in widths],
            *[V((5, planes + w - 2, side, columns), F32) for w in widths],
            *[V((5, planes + w - 2, side, columns), F32) for w in widths],
            V((3, planes, columns // 128, rows, 128), F32),
            V((lines, cols), BF16), V((devices, 1, lanes), jnp.int32), V((devices, 1, lanes), jnp.int32),
            V((lines, 2 * lanes), BF16),
            V((cols, half), BF16), V((cols, half), BF16),
            V((STEPS, lines, half), F32), V((STEPS, lines, half), F32),
            V((3 * n, n, n, lanes), F32),
            V((n, n, n, lanes), F32), V((2, n, n, lanes), F32), V((n, n, lanes), F32),
            V((5,) + wave_shape, F32),
            V((stages, 2, n, n, lanes), F32), V((stages, 2, n, n, lanes), F32),
            DMA((5,)), DMA((stages, 4)), DMA((stages, 4)),
            DMA((stages, 2, planes + 6)), DMA((stages, 2, planes + 6)),
            DMA((stages, 2)), DMA((stages, 2)), DMA(()), DMA(()),
            DMA((STEPS,)), DMA((STEPS,)),
        ],
        compiler_params=pltpu.CompilerParams(
            collective_id=0, has_side_effects=True, vmem_limit_bytes=58000 * 1024
        ),
        name="march",
    )(*[pltpu.with_memory_space_constraint(v, pltpu.HBM) for v in (density, velocity, pressure, wave_state, tables)], margin_element, margin_block, margin_table)
    fields, wave, forcing = put_out(fields, wave, forcing)
    return fields, wave, forcing.reshape((3, n, n, n, lanes))


def solution(mesh):
    in_specs = (
        P("flow", "group", None),
        P(None, "flow", "group", None),
        P("flow", "group", None),
        P(None, None, None, None, ("flow", "group")),
        P(),
        P(("flow", "group"), None),
        P(("flow", "group"), None),
        P(("flow", "group"), None),
    )
    out_specs = (
        P(None, "flow", "group", None),
        P(None, None, None, None, ("flow", "group")),
        P(None, None, None, None, ("flow", "group")),
    )
    return jax.shard_map(local, mesh=mesh, in_specs=in_specs, out_specs=out_specs, check_vma=False)
```

```python
import jax
import jax.numpy as jnp
import numpy as np
from jax import lax
from jax.experimental import pallas as pl
from jax.experimental.pallas import tpu as pltpu
from jax.sharding import PartitionSpec as P

EZ = 16
CAP = 4
STEPS = 2

GAMMA = 1.4
DT_FLOW = 0.08
ACOUSTIC_STEP = 0.01
F32, BF16 = jnp.float32, jnp.bfloat16
KEEP = (0.0, 0.75, 1.0 / 3.0)
GAIN = (1.0, 0.25, 2.0 / 3.0)


def legendre_pair(quadrature_nodes, degree):
    previous = np.ones(quadrature_nodes.shape[0])
    current = quadrature_nodes * 1.0
    for order in range(2, degree + 1):
        previous, current = (
            current,
            ((2 * order - 1) * quadrature_nodes * current - (order - 1) * previous) / order,
        )
    return (previous, current)


def lobatto(point_count):
    degree = point_count - 1
    quadrature_nodes = -np.cos(np.pi * np.arange(point_count) / degree)
    for sweep in range(60):
        previous, current = legendre_pair(quadrature_nodes, degree)
        quadrature_nodes = quadrature_nodes - (quadrature_nodes * current - previous) / (
            point_count * current
        )
    previous, values = legendre_pair(quadrature_nodes, degree)
    quadrature_weights = 2.0 / (degree * (degree + 1) * values**2)
    identity = np.eye(point_count)
    differ = quadrature_nodes[:, None] - quadrature_nodes[None, :] + identity
    matrix = values[:, None] / values[None, :] / differ * (1.0 - identity)
    matrix[0, 0] = -degree * (degree + 1) / 4.0
    matrix[-1, -1] = degree * (degree + 1) / 4.0
    return (matrix, float(quadrature_weights[0]))


def iota(shape, axis):
    return lax.broadcasted_iota(jnp.int32, shape, axis)


def split(value):
    high = value.astype(BF16)
    return high, (value - high.astype(F32)).astype(BF16)


def dot(a, b):
    return jnp.dot(a, b, preferred_element_type=F32)


def primitive(state):
    inverse = 1.0 / state[0]
    vel = [state[1 + d] * inverse for d in range(3)]
    square = vel[0] * vel[0] + vel[1] * vel[1] + vel[2] * vel[2]
    pressure = (GAMMA - 1.0) * (state[4] - 0.5 * state[0] * square)
    return vel, pressure, jnp.sqrt(GAMMA * pressure * inverse)


def flux_of(state, prim, d):
    vel, pressure, sound = prim
    normal = vel[d]
    parts = [state[0] * normal]
    for c in range(3):
        product = state[1 + c] * normal
        parts.append(product + pressure if c == d else product)
    parts.append((state[4] + pressure) * normal)
    return parts, jnp.abs(normal) + sound


def face(left, right, left_flux, right_flux, left_speed, right_speed):
    speed = jnp.maximum(left_speed, right_speed)
    return [
        0.5 * (left_flux[c] + right_flux[c]) - 0.5 * speed * (right[c] - left[c])
        for c in range(5)
    ]


def along(cell, prim, d, axis):
    size = cell[0].shape[axis]
    flux, speed = flux_of(cell, prim, d)
    back = lambda v: pltpu.roll(v, size - 1, axis)
    upper = face(
        cell, [back(v) for v in cell], flux, [back(v) for v in flux], speed, back(speed)
    )
    return [upper[c] - pltpu.roll(upper[c], 1, axis) for c in range(5)]


def tall_of(own, above, below):
    row = iota(above.shape, 0)
    return jnp.concatenate([own, jnp.where(row < above.shape[0] // 2, above, below)], axis=0)


def flow_stage(src, above, below, finish, before, after):
    planes, rows = src.shape[1] - 2, src.shape[2]

    def load(p):
        return [src[c, p] for c in range(5)]

    def x_side(p):
        cell = load(p)
        flux, speed = flux_of(cell, primitive(cell), 0)
        return cell, flux, speed

    def x_face(p):
        left, right = x_side(p), x_side(p + 1)
        return face(left[0], right[0], left[1], right[1], left[2], right[2])

    def body(p, lower):
        before(p)
        upper = x_face(p + 1)
        tall = [tall_of(src[c, p + 1], above[c, p], below[c, p]) for c in range(5)]
        prim = primitive(tall)
        dy = along(tall, prim, 1, 0)
        cell = [v[:rows] for v in tall]
        prim = ([v[:rows] for v in prim[0]], prim[1][:rows], prim[2][:rows])
        dz = along(cell, prim, 2, 1)
        for c in range(5):
            rate = -(upper[c] - lower[c]) - dy[c][:rows] - dz[c]
            finish(p, c, cell[c] + DT_FLOW * rate)
        after(p)
        return tuple(upper)

    lax.fori_loop(0, planes, body, tuple(x_face(0)))


def lamb(src, above, below, out):
    planes, rows, columns = src.shape[1] - 2, src.shape[2], src.shape[3]

    def body(p, _):
        density = tall_of(src[0, p + 1], above[0, p], below[0, p])
        inverse = 1.0 / density
        tall = [
            tall_of(src[1 + d, p + 1], above[1 + d, p], below[1 + d, p]) * inverse
            for d in range(3)
        ]
        size = tall[0].shape[0]
        slope_y = [
            0.5 * (pltpu.roll(v, size - 1, 0) - pltpu.roll(v, 1, 0))[:rows] for v in tall
        ]
        vel = [v[:rows] for v in tall]
        slope_z = [0.5 * (pltpu.roll(v, columns - 1, 1) - pltpu.roll(v, 1, 1)) for v in vel]
        after, before = 1.0 / src[0, p + 2], 1.0 / src[0, p]
        slope_x = [
            0.5 * (src[1 + d, p + 2] * after - src[1 + d, p] * before) for d in range(3)
        ]
        curl_x = slope_y[2] - slope_z[1]
        curl_y = slope_z[0] - slope_x[2]
        curl_z = slope_x[1] - slope_y[0]
        result = [
            curl_y * vel[2] - curl_z * vel[1],
            curl_z * vel[0] - curl_x * vel[2],
            curl_x * vel[1] - curl_y * vel[0],
        ]
        for d in range(3):
            for q in range(out.shape[2]):
                out[d, p, q] = result[d][:, q * 128 : (q + 1) * 128]
        return 0

    lax.fori_loop(0, planes, body, 0)


def split_tables(tables, high, low):
    count, depth, _ = tables.shape
    step = 64

    def body(i, _):
        t = i // (depth // step)
        at = pl.ds(pl.multiple_of((i % (depth // step)) * step, step), step)
        h, l = split(tables[t, at, :])
        high[t, at, :] = h
        low[t, at, :] = l
        return 0

    lax.fori_loop(0, count * (depth // step), body, 0)


def rows_of_slots(source, high, low, pick, mapped_high, mapped_low, send):
    _, planes, chunks, rows, width = source.shape
    columns = chunks * width
    table_count, depth, nodes = high.shape
    per = depth // columns
    strip = rows // per
    blocks = planes * strip
    half = 3 * nodes // 2
    pieces = []
    for y in range(3):
        for p in range(planes):
            pieces.append(
                jnp.concatenate(
                    [
                        source[y, p, q, pl.ds(r, strip, stride=per), :]
                        for r in range(per)
                        for q in range(chunks)
                    ],
                    axis=1,
                )
            )
    left_high, left_low = split(jnp.concatenate(pieces, axis=0))
    both = jnp.concatenate([left_high, left_low], axis=0)
    count = 3 * blocks

    def body(t, _):
        wide = dot(both, high[t])
        out = wide[:count] + wide[count:] + dot(left_high, low[t])
        for side in range(2):
            at = pl.ds(pl.multiple_of(side * table_count * blocks + t * blocks, blocks), blocks)
            for y in range(3):
                begin, end = max(y * nodes, side * half), min((y + 1) * nodes, (side + 1) * half)
                if begin < end:
                    value = out[y * blocks : (y + 1) * blocks, begin - y * nodes : end - y * nodes]
                    h, l = split(value)
                    mapped_high[at, begin - side * half : end - side * half] = h
                    mapped_low[at, begin - side * half : end - side * half] = l
        return 0

    lax.fori_loop(0, table_count, body, 0)
    send[...] = dot(pick[...], mapped_high[...]) + dot(pick[...], mapped_low[...])


def routes(element, block, table, blocks, table_count, local_count, devices, pick, label):
    entries = element.shape[1]
    shift = local_count.bit_length() - 1
    assert 1 << shift == local_count
    owner = lax.shift_right_logical(element, shift)
    local_index = element - lax.shift_left(owner, shift)
    column = table * blocks + block
    square = (entries, entries)
    row = jnp.broadcast_to(owner, square)
    turned = jnp.sum(jnp.where(iota(square, 0) == iota(square, 1), row, 0), axis=1, keepdims=True)
    earlier = (turned == row) & (iota(square, 0) < iota(square, 1))
    rank = jnp.sum(jnp.where(earlier, 1, 0), axis=0, keepdims=True)
    slot = owner * CAP + rank
    high = 2 * CAP
    lines = devices * high
    line = iota((lines, entries), 0)
    named = (line // high) * CAP + line % CAP
    hit = named == slot
    labels = jnp.sum(jnp.where(hit, local_index + 1, 0), axis=1, keepdims=True) - 1
    picked = jnp.sum(jnp.where(hit, column + 1, 0), axis=1, keepdims=True) - 1
    tiles = (devices, high, label.shape[2])
    spread = jnp.broadcast_to(labels, (lines, tiles[2])).reshape(tiles)
    label[...] = jnp.sum(
        jnp.where(iota(tiles, 1) == iota(tiles, 2), spread, 0), axis=1, keepdims=True
    )
    shape = pick.shape
    side = (iota(shape, 0) // CAP) % 2
    chosen = picked + side * (table_count * blocks)
    on = (iota(shape, 1) == chosen) & (picked >= 0)
    pick[...] = jnp.where(on, 1.0, 0.0).astype(BF16)


def place_of(label, place):
    devices, _, lanes = label.shape
    high = 2 * CAP
    shape = (devices * high, lanes)
    wide = jnp.broadcast_to(label[...], (devices, high, lanes)).reshape(shape)
    line, lane = iota(shape, 0), iota(shape, 1)
    named = jnp.sum(jnp.where(line % CAP == lane, wide, 0), axis=1, keepdims=True)
    side = (line // CAP) % 2
    hit = named == lane
    for s in range(2):
        place[:, s * lanes : (s + 1) * lanes] = jnp.where(hit & (side == s), 1.0, 0.0).astype(BF16)


def add_up(received, place, forcing):
    parts, lanes = forcing.shape[0] // 2, forcing.shape[-1]
    high, low = split(received[...].T)
    total = dot(high, place[...]) + dot(low, place[...])
    for s in range(2):
        forcing[s * parts : (s + 1) * parts] = total[:, s * lanes : (s + 1) * lanes].reshape(
            (parts,) + forcing.shape[1:]
        )


def halves(matrix):
    n = matrix.shape[0]
    turned = matrix[: n // 2, ::-1][:, : n // 2]
    own = matrix[: n // 2, : n // 2]
    return 0.5 * (own + turned), 0.5 * (own - turned)


def derive(values, even, odd):
    n = len(values)
    h = n // 2
    sums = [values[m] + values[n - 1 - m] for m in range(h)]
    gaps = [values[m] - values[n - 1 - m] for m in range(h)]
    out = [None] * n
    for a in range(h):
        alpha = sum(float(even[a, m]) * sums[m] for m in range(h))
        beta = sum(float(odd[a, m]) * gaps[m] for m in range(h))
        out[a] = beta + alpha
        out[n - 1 - a] = beta - alpha
    return out


def wave_main(start, cur, forcing, out, partial, edge, dcol, matrix, lift, stage, forced):
    keep, gain = KEEP[stage], GAIN[stage]
    n, lanes = cur.shape[1], cur.shape[-1]
    last = n - 1
    even, odd = halves(matrix)
    node = iota((n, lanes), 0)
    z = iota((n, lanes), 1) % EZ
    turn = lambda v, by: pltpu.roll(v, by % lanes, v.ndim - 1)

    def store(f, i, j, rate):
        value = gain * cur[f, i, j] + (gain * ACOUSTIC_STEP) * rate
        if keep:
            value = keep * start[f, i, j] + value
        out[f, i, j] = value

    def push(d, i, j):
        return forcing[d * n + i, j] if forced else 0.0

    def edges(i, _):
        p7, u7 = cur[0, i, :, last, :], cur[3, i, :, last, :]
        p0, u0 = cur[0, i, :, 0, :], cur[3, i, :, 0, :]
        plus, minus = u7 + p7, u0 - p0
        below = jnp.where(z == 0, turn(plus, 1 - EZ), turn(plus, 1))
        above = jnp.where(z == EZ - 1, turn(minus, EZ - 1), turn(minus, -1))
        edge[0, i] = lift * (below - (u0 + p0))
        edge[1, i] = lift * (above - (u7 - p7))
        return 0

    lax.fori_loop(0, n, edges, 0)

    def lines_i(j, _):
        d_u = derive([cur[1, i, j] for i in range(n)], even, odd)
        d_p = derive([cur[0, i, j] for i in range(n)], even, odd)
        for i in range(n):
            store(1, i, j, push(0, i, j) - d_p[i])
            rate_p, rate_w = d_u[i], 0.0
            for m in range(n):
                rate_p = rate_p + dcol[m] * cur[3, i, j, m : m + 1, :]
                rate_w = rate_w + dcol[m] * cur[0, i, j, m : m + 1, :]
            low = jnp.where(node == 0, edge[0, i, pl.ds(j, 1), :], 0.0)
            up = jnp.where(node == last, edge[1, i, pl.ds(j, 1), :], 0.0)
            partial[i, j] = (low - up) - rate_p
            store(3, i, j, push(2, i, j) + ((low + up) - rate_w))
        return 0

    lax.fori_loop(0, n, lines_i, 0)

    def lines_j(i, _):
        p = [cur[0, i, j] for j in range(n)]
        v = [cur[2, i, j] for j in range(n)]
        low = lift * (turn(v[last] + p[last], EZ) - (v[0] + p[0]))
        up = lift * (turn(v[0] - p[0], -EZ) - (v[last] - p[last]))
        d_v = derive(v, even, odd)
        d_p = derive(p, even, odd)
        for j in range(n):
            rate_p, rate_v = partial[i, j] - d_v[j], push(1, i, j) - d_p[j]
            if j == 0:
                rate_p, rate_v = rate_p + low, rate_v + low
            if j == last:
                rate_p, rate_v = rate_p - up, rate_v + up
            store(0, i, j, rate_p)
            store(2, i, j, rate_v)
        return 0

    lax.fori_loop(0, n, lines_j, 0)


def wave_force(out, forcing, stage):
    n = out.shape[1]
    scale = GAIN[stage] * ACOUSTIC_STEP

    def body(i, _):
        for d in range(3):
            out[1 + d, i] = out[1 + d, i] + scale * forcing[d * n + i]
        return 0

    lax.fori_loop(0, n, body, 0)


def wave_faces(cur, out, below, above, lift, stage):
    last = cur.shape[1] - 1
    scale = GAIN[stage] * ACOUSTIC_STEP * lift
    low = scale * (below[...] - (cur[1, 0] + cur[0, 0]))
    out[0, 0] = out[0, 0] + low
    out[1, 0] = out[1, 0] + low
    up = scale * (above[...] - (cur[1, last] - cur[0, last]))
    out[0, last] = out[0, last] - up
    out[1, last] = out[1, last] + up


def all_kernel(
    sizes, den_hbm, vel_hbm, pre_hbm, wave_hbm, tables_hbm, element, block, table,
    fields_out, wave_out, forcing_out,
    den, vel, pre, wave0, tables, high, low, X0, X1, X2, X3, X4, X5,
    A0, A1, A2, A3, A4, A5, B0, B1, B2, B3, B4, B5, S, pick, label, label_in, place,
    mapped_high, mapped_low, send, recv, forcing1, partial, edge, dcol, V, FS, FR,
    local_sem, x_send, x_recv, y_send, y_recv, w_send, w_recv, l_send, l_recv, a_send, a_recv,
):
    flows, groups, local_count = sizes
    devices = flows * groups
    planes, rows, columns = den.shape
    f, g = lax.axis_index("flow"), lax.axis_index("group")
    me = f * groups + g
    at = lambda k: (k // groups, k % groups)
    matrix, end_weight = lobatto(wave0.shape[1])
    lift = 0.5 / end_weight
    n = wave0.shape[1]

    loads = [
        pltpu.make_async_copy(a, b, local_sem.at[i])
        for i, (a, b) in enumerate(
            [(den_hbm, den), (vel_hbm, vel), (pre_hbm, pre), (wave_hbm, wave0), (tables_hbm, tables)]
        )
    ]
    for c in loads:
        c.start()
    barrier = pltpu.get_barrier_semaphore()

    def greet(d, _):
        pl.semaphore_signal(
            barrier, inc=1, device_id=at((me + d) % devices), device_id_type=pl.DeviceIdType.MESH
        )
        return 0

    lax.fori_loop(1, devices, greet, 0)

    pending = []

    def remote(src, dst, ssem, rsem, device):
        c = pltpu.make_async_remote_copy(
            src_ref=src, dst_ref=dst, send_sem=ssem, recv_sem=rsem,
            device_id=device, device_id_type=pl.DeviceIdType.MESH,
        )
        c.start()
        pending.append(c)
        return c

    X = [X0, X1, X2, X3, X4, X5]
    A, B = [A0, A1, A2, A3, A4, A5], [B0, B1, B2, B3, B4, B5]
    r8 = A0.shape[2]
    up_g, down_g = (f, (g + 1) % groups), (f, (g + groups - 1) % groups)
    up_f, down_f = ((f + 1) % flows, g), ((f + flows - 1) % flows, g)

    def y_copies(s, p):
        return [
            pltpu.make_async_remote_copy(
                src_ref=X[s].at[:, p + 1, band], dst_ref=ghost[s].at[:, p],
                send_sem=y_send.at[s, way, p], recv_sem=y_recv.at[s, way, p],
                device_id=device, device_id_type=pl.DeviceIdType.MESH,
            )
            for way, (band, ghost, device) in enumerate(
                [(slice(0, r8), A, down_g), (slice(rows - r8, rows), B, up_g)]
            )
        ]

    def send_y(s, p):
        for c in y_copies(s, p):
            c.start()

    def wait_y(s, p):
        for c in y_copies(s, p):
            c.wait_recv()

    def over(begin, end, do):
        def body(p, _):
            do(p)
            return 0
        lax.fori_loop(begin, end, body, 0)

    def send_x(s, i, low, low_to, high, high_to):
        return [
            remote(X[s].at[:, low], X[s].at[:, low_to], x_send.at[s, i], x_recv.at[s, i], down_f),
            remote(X[s].at[:, high], X[s].at[:, high_to], x_send.at[s, i + 1], x_recv.at[s, i + 1], up_f),
        ]

    def send_halos(s):
        return send_x(s, 0, slice(1, 2), slice(planes + 1, planes + 2), slice(planes, planes + 1), slice(0, 1))

    def send_faces(s, cur):
        last = n - 1
        FS[s, 0] = cur[1, last] + cur[0, last]
        FS[s, 1] = cur[1, 0] - cur[0, 0]
        return [
            remote(FS.at[s, 0], FR.at[s, 0], w_send.at[s, 0], w_recv.at[s, 0], at((me + 1) % devices)),
            remote(FS.at[s, 1], FR.at[s, 1], w_send.at[s, 1], w_recv.at[s, 1], at((me + devices - 1) % devices)),
        ]

    def arrive(copies):
        for c in copies:
            c.wait_recv()

    high_rows = 2 * CAP

    def slot_copy(src, dst, ssem, rsem, peer, owner):
        size = src.shape[0] // devices
        block_at = lambda k: pl.ds(pl.multiple_of(k * size, size), size)
        return pltpu.make_async_remote_copy(
            src_ref=src.at[block_at(peer)], dst_ref=dst.at[block_at(owner)],
            send_sem=ssem, recv_sem=rsem,
            device_id=at(peer), device_id_type=pl.DeviceIdType.MESH,
        )

    stride = 5 if np.gcd(5, devices) == 1 else 1

    def exchange(src, dst, ssem, rsem, begin, end):
        def body(k, _):
            slot_copy(src, dst, ssem, rsem, (me + k * stride) % devices, me).start()
            return 0
        lax.fori_loop(begin, end, body, 0)

    def keep_own(src, dst):
        size = src.shape[0] // devices
        mine = pl.ds(pl.multiple_of(me * size, size), size)
        dst[mine] = src[mine]

    def all_blocks(src, dst, ssem, rsem):
        others = pl.ds(0, (devices - 1) * (src.shape[0] // devices))
        return pltpu.make_async_remote_copy(
            src_ref=src.at[others], dst_ref=dst.at[others], send_sem=ssem, recv_sem=rsem,
            device_id=at((me + 1) % devices), device_id_type=pl.DeviceIdType.MESH,
        )

    def settle(*refs):
        all_blocks(*refs).wait_recv()

    def drain(*refs):
        all_blocks(*refs).wait_send()

    for c in loads[:3]:
        c.wait()

    deep = 4
    assert planes == deep and flows % 2 == 0

    def conserve(p, _):
        r = den[p]
        v = [vel[d, p] for d in range(3)]
        X0[0, p + deep] = r
        for d in range(3):
            X0[1 + d, p + deep] = r * v[d]
        square = v[0] * v[0] + v[1] * v[1] + v[2] * v[2]
        X0[4, p + deep] = pre[p] / (GAMMA - 1.0) + 0.5 * r * square
        return 0

    lax.fori_loop(0, planes, conserve, 0)
    pl.semaphore_wait(barrier, devices - 1)
    near = send_x(
        0, 0, slice(deep, deep + 1), slice(deep + planes, deep + planes + 1),
        slice(deep + planes - 1, deep + planes), slice(deep - 1, deep),
    )
    over(deep - 1, deep - 1 + planes, lambda p: send_y(0, p))
    odd = f % 2
    partner = ((f + 1 - 2 * odd) % flows, g)
    beyond = ((f + 2 - 4 * odd + flows) % flows, g)
    pick_by = lambda even_value, odd_value: even_value + odd * (odd_value - even_value)

    def x_plane(src, dst, i, device):
        return pltpu.make_async_remote_copy(
            src_ref=X0.at[:, pl.ds(src, 1)], dst_ref=X0.at[:, pl.ds(dst, 1)],
            send_sem=x_send.at[0, i], recv_sem=x_recv.at[0, i],
            device_id=device, device_id_type=pl.DeviceIdType.MESH,
        )

    def direct(d):
        return x_plane(
            pick_by(deep + planes - d, deep + d - 1), pick_by(deep - d, deep + planes + d - 1),
            d, partner,
        )

    def onward(d):
        return x_plane(
            pick_by(deep + planes + d - 1, deep - d),
            pick_by(deep - planes + d - 1, deep + 2 * planes - d), deep + d, beyond,
        )

    def near_of(side):
        return pltpu.make_async_remote_copy(
            src_ref=X0.at[:, 0:1], dst_ref=X0.at[:, 0:1],
            send_sem=x_send.at[0, side], recv_sem=x_recv.at[0, side],
            device_id=partner, device_id_type=pl.DeviceIdType.MESH,
        )

    for d in range(2, deep + 1):
        direct(d).start()

    def pass_on(d):
        if d == 1:
            near_of(odd).wait_recv()
        else:
            direct(d).wait_recv()
        onward(d).start()

    loads[3].wait()
    waves = send_faces(0, wave0)
    blocks = planes * rows * columns // tables.shape[1]
    routes(element[...], block[...], table[...], blocks, tables.shape[0], local_count, devices, pick, label)
    exchange(label, label_in, l_send, l_recv, 1, devices)
    keep_own(label, label_in)
    row = iota((n, dcol.shape[-1]), 0)
    for m in range(n):
        tile = jnp.zeros((n, dcol.shape[-1]), F32)
        for k in range(n):
            tile = jnp.where(row == k, float(matrix[k, m]), tile)
        dcol[m] = tile
    loads[4].wait()
    split_tables(tables, high, low)

    forcings = [forcing1, forcing_out]
    def flow_part(s):
        step, stage = s // 3, s % 3
        base = 3 * step
        lag = 1 if s >= 3 else 0
        total = X[s].shape[1] - 2

        def finish(p, c, value):
            if stage:
                value = KEEP[stage] * X[base][c, p + (stage + 1 if s < 3 else 1)] + GAIN[stage] * value
            if s == 3 * STEPS - 1:
                fields_out[c, p] = value
            else:
                X[s + 1][c, p + lag] = value

        def before(p):
            if s not in (0, 3):
                wait_y(s, p)

        def after(p):
            if s == 3 * STEPS - 1:
                return
            first = 1 if lag else 2

            @pl.when((p >= first) & (p - first < X[s + 1].shape[1] - 2))
            def _():
                send_y(s + 1, p - first)

        flow_stage(X[s], A[s], B[s], finish, before, after)
        if lag and s < 3 * STEPS - 1:
            send_y(s + 1, total - 1)

    def project(step):
        rows_of_slots(S, high, low, pick, mapped_high, mapped_low, send.at[step])
        keep_own(send.at[step], recv.at[step])

    def issue(step, begin, end):
        cut = lambda t: 1 + int(round(t * (devices - 1)))
        exchange(send.at[step], recv.at[step], a_send.at[step], a_recv.at[step], cut(begin), cut(end))

    curs = [wave0] + [V.at[i] for i in range(5)] + [wave_out]

    def main(s, forced):
        step, stage = s // 3, s % 3
        wave_main(curs[3 * step], curs[s], forcings[step], curs[s + 1], partial, edge, dcol,
                  matrix, lift, stage, forced)

    def finish_wave(s, copies):
        arrive(copies)
        wave_faces(curs[s], curs[s + 1], FR.at[s, 0], FR.at[s, 1], lift, s % 3)

    main(0, False)
    pass_on(1)
    near_of(1 - odd).wait_recv()
    over(deep - 1, deep - 1 + planes, lambda p: wait_y(0, p))
    mid, own = pl.ds(deep - 1, planes + 2), pl.ds(deep - 1, planes)
    lamb(X0.at[:, mid], A0.at[:, own], B0.at[:, own], S)
    pass_on(2)
    project(0)
    pass_on(3)
    issue(0, 0.0, 1.0)
    direct(deep).wait_recv()
    for d in range(1, deep):
        onward(d).wait_recv()
    for part in ((0, deep - 1), (deep - 1 + planes, 2 * deep + planes - 2)):
        over(*part, lambda p: send_y(0, p))
    for part in ((0, deep - 1), (deep - 1 + planes, 2 * deep + planes - 2)):
        over(*part, lambda p: wait_y(0, p))
    flow_part(0)
    flow_part(1)
    flow_part(2)
    over(0, planes, lambda p: wait_y(3, p))
    flow_part(3)
    halo = send_halos(4)
    lamb(X3, A3, B3, S)
    project(1)
    issue(1, 0.0, 0.2)
    settle(label, label_in, l_send, l_recv)
    place_of(label_in, place)
    settle(send.at[0], recv.at[0], a_send.at[0], a_recv.at[0])
    add_up(recv.at[0], place, forcing1)
    finish_wave(0, waves)
    wave_force(curs[1], forcing1, 0)
    waves = send_faces(1, curs[1])
    issue(1, 0.2, 0.6)
    main(1, True)
    finish_wave(1, waves)
    waves = send_faces(2, curs[2])
    arrive(halo)
    flow_part(4)
    halo = send_halos(5)
    issue(1, 0.6, 0.9)
    main(2, True)
    finish_wave(2, waves)
    waves = send_faces(3, curs[3])
    issue(1, 0.9, 1.0)
    main(3, False)
    arrive(halo)
    flow_part(5)
    for s in range(3 * STEPS):
        def drained(p, s=s):
            for c in y_copies(s, p):
                c.wait_send()
        over(0, X[s].shape[1] - 2, drained)
    drain(label, label_in, l_send, l_recv)
    for d in range(1, deep):
        direct(d + 1).wait_send()
        onward(d).wait_send()
    drain(send.at[0], recv.at[0], a_send.at[0], a_recv.at[0])
    settle(send.at[1], recv.at[1], a_send.at[1], a_recv.at[1])
    add_up(recv.at[1], place, forcing_out)
    finish_wave(3, waves)
    wave_force(curs[4], forcing_out, 0)
    waves = send_faces(4, curs[4])
    main(4, True)
    finish_wave(4, waves)
    waves = send_faces(5, curs[5])
    main(5, True)
    drain(send.at[1], recv.at[1], a_send.at[1], a_recv.at[1])
    finish_wave(5, waves)
    for c in pending:
        c.wait_send()


def put_out(*values):
    count = len(values)

    def body(*refs):
        copies = [
            pltpu.make_async_copy(refs[i], refs[count + i], refs[2 * count].at[i])
            for i in range(count)
        ]
        for c in copies:
            c.start()
        for c in copies:
            c.wait()

    return pl.pallas_call(
        body,
        out_shape=tuple(jax.ShapeDtypeStruct(v.shape, v.dtype) for v in values),
        in_specs=[pl.BlockSpec(memory_space=pltpu.VMEM)] * count,
        out_specs=tuple([pl.BlockSpec(memory_space=pl.ANY)] * count),
        scratch_shapes=[pltpu.SemaphoreType.DMA((count,))],
        name="put_out",
    )(*[pltpu.with_memory_space_constraint(v, pltpu.VMEM) for v in values])


def local(
    density, velocity, pressure, wave_state, tables, margin_element, margin_block, margin_table
):
    flows, groups = lax.axis_size("flow"), lax.axis_size("group")
    devices = flows * groups
    planes, rows, columns = density.shape
    n, lanes = wave_state.shape[1], wave_state.shape[-1]
    table_count, depth, nodes = tables.shape
    blocks = density.size // depth
    lines = devices * 2 * CAP
    half = 3 * nodes // 2
    cols = 2 * table_count * blocks
    stages = 3 * STEPS
    side = 8
    widths = (8, 6, 4, 2, 2, 2)
    any_spec = pl.BlockSpec(memory_space=pltpu.HBM)
    vmem = pl.BlockSpec(memory_space=pltpu.VMEM)
    V = pltpu.VMEM
    DMA = pltpu.SemaphoreType.DMA
    wave_shape = wave_state.shape

    def body(*refs):
        all_kernel((flows, groups, lanes), *refs)

    fields, wave, forcing = pl.pallas_call(
        body,
        out_shape=(
            V((5, planes, rows, columns), F32),
            V(wave_shape, F32),
            V((3 * n, n, n, lanes), F32),
        ),
        in_specs=[any_spec] * 5 + [vmem] * 3,
        out_specs=(vmem, vmem, vmem),
        scratch_shapes=[
            V((planes, rows, columns), F32), V((3, planes, rows, columns), F32),
            V((planes, rows, columns), F32), V(wave_shape, F32), V(tables.shape, F32),
            V(tables.shape, BF16), V(tables.shape, BF16),
            *[V((5, planes + w, rows, columns), F32) for w in widths],
            *[V((5, planes + w - 2, side, columns), F32) for w in widths],
            *[V((5, planes + w - 2, side, columns), F32) for w in widths],
            V((3, planes, columns // 128, rows, 128), F32),
            V((lines, cols), BF16), V((devices, 1, lanes), jnp.int32), V((devices, 1, lanes), jnp.int32),
            V((lines, 2 * lanes), BF16),
            V((cols, half), BF16), V((cols, half), BF16),
            V((STEPS, lines, half), F32), V((STEPS, lines, half), F32),
            V((3 * n, n, n, lanes), F32),
            V((n, n, n, lanes), F32), V((2, n, n, lanes), F32), V((n, n, lanes), F32),
            V((5,) + wave_shape, F32),
            V((stages, 2, n, n, lanes), F32), V((stages, 2, n, n, lanes), F32),
            DMA((5,)), DMA((stages, 8)), DMA((stages, 8)),
            DMA((stages, 2, planes + 6)), DMA((stages, 2, planes + 6)),
            DMA((stages, 2)), DMA((stages, 2)), DMA(()), DMA(()),
            DMA((STEPS,)), DMA((STEPS,)),
        ],
        compiler_params=pltpu.CompilerParams(
            collective_id=0, has_side_effects=True, vmem_limit_bytes=58000 * 1024
        ),
        name="march",
    )(*[pltpu.with_memory_space_constraint(v, pltpu.HBM) for v in (density, velocity, pressure, wave_state, tables)], margin_element, margin_block, margin_table)
    fields, wave, forcing = put_out(fields, wave, forcing)
    return fields, wave, forcing.reshape((3, n, n, n, lanes))


def solution(mesh):
    in_specs = (
        P("flow", "group", None),
        P(None, "flow", "group", None),
        P("flow", "group", None),
        P(None, None, None, None, ("flow", "group")),
        P(),
        P(("flow", "group"), None),
        P(("flow", "group"), None),
        P(("flow", "group"), None),
    )
    out_specs = (
        P(None, "flow", "group", None),
        P(None, None, None, None, ("flow", "group")),
        P(None, None, None, None, ("flow", "group")),
    )
    return jax.shard_map(local, mesh=mesh, in_specs=in_specs, out_specs=out_specs, check_vma=False)
```
